32 devices in a mesh: sp: 2 (over core), py: 4 (over z), pz: 4 (over y, x).
Axes of the slice: x: 2, y: 2, z: 4, core: 2. Of those that a mesh axis runs over, the one named last changes fastest.
Arguments:
- concentration: float32 [8, 128, 128, 128], P('sp', 'py', 'pz'), may hold values from -1 to 1.1
- mobility: float32 [8, 8], replicated, may hold values from 0.1 to 0.6
- kappa: float32 [8], replicated, may hold values from 0.5 to 2
- well_depth: float32 [8], P('sp'), may hold values from 0.5 to 2
Outputs:
- updated: float32 [8, 128, 128, 128], P('sp', 'py', 'pz')
The draws below stay inside these ranges and needn't reach their ends.
All inputs are finite; a program needn't handle non-finite values.
Results may differ from the reference program's by a relative error of at most 0.000084.
Values sent between devices are 32-bit elements; how exact they have to be, the bound alone decides.
A program may use at most 128 MiB of HBM per device.

```python
import math
import jax
import jax.numpy as jnp
from jax import lax

S = 8
NX = 128
NY = 128
NZ = 128


def draw_concentration(key, part):
    first = jax.random.fold_in(jax.random.fold_in(key, 11), 0)
    base = jax.random.uniform(first, (S, NX, NY, NZ), jnp.float32, -1.0, 1.0)
    return base


def level_of(own_key, extent, cuts, least, top_value):
    factor_of = 1.0
    for position, shards_of in cuts:
        draws = jax.random.uniform(jax.random.fold_in(jax.random.fold_in(own_key, 6), position), (shards_of,), jnp.float32, least / len(cuts), top_value / len(cuts))
        factor_of = factor_of * jnp.repeat(jnp.exp(draws), extent[position] // shards_of).reshape((-1,) + (1,) * (len(extent) - 1 - position))
    return factor_of


def setup_inputs(seed: int = 0) -> dict:
    seeds = jax.random.split(jax.random.key(seed), 5)
    return {
        "concentration": draw_concentration(jax.random.fold_in(seeds[4], 71), 0),
        "mobility": jnp.clip(jax.random.uniform(seeds[1], (S, S), jnp.float32, 0.1, 0.6), 0.1, 0.6),
        "kappa": jnp.clip(jnp.exp(jax.random.uniform(seeds[2], (S,), jnp.float32, math.log(0.5), math.log(2.0))), 0.5, 2.0),
        "well_depth": jnp.clip(jnp.exp(math.log(2.0) - 1.3862944 * jax.random.uniform(seeds[3], (S,), jnp.float32) ** level_of(seeds[3], (S,), ((0, 2),), -0.2, 0.2)), 0.5, 2.0),
    }


def wave_square(count):
    modes = jnp.arange(count, dtype=jnp.int32)
    freq = jnp.where(modes < count // 2, modes, modes - count).astype(jnp.float32)
    return (2.0 * math.pi * freq / count) ** 2


def reference(concentration, mobility, kappa, well_depth):
    conc = concentration
    bulk = well_depth[:, None, None, None] * (conc * conc * conc - conc)
    c_hat = jnp.fft.fftn(conc, axes=(1, 2, 3))
    bulk_hat = jnp.fft.fftn(bulk, axes=(1, 2, 3))
    ksq = wave_square(NX)[:, None, None] + wave_square(NY)[None, :, None] + wave_square(NZ)[None, None, :]
    drive = bulk_hat + kappa[:, None, None, None] * ksq[None] * c_hat
    mix_real = jnp.einsum("ij,jxyz->ixyz", mobility, jnp.real(drive), precision=lax.Precision.HIGHEST)
    mix_imag = jnp.einsum("ij,jxyz->ixyz", mobility, jnp.imag(drive), precision=lax.Precision.HIGHEST)
    mix = mix_real + 1j * mix_imag
    stiff = 0.5 * (jnp.diagonal(mobility) * kappa)[:, None, None, None] * (ksq * ksq)[None]
    new_hat = (c_hat * (1.0 + stiff) - 0.5 * ksq[None] * mix) / (1.0 + stiff)
    updated = jnp.real(jnp.fft.ifftn(new_hat, axes=(1, 2, 3)))
    return updated.astype(jnp.float32)
```

```python
import functools
import math

import jax
import jax.numpy as jnp
import numpy as np
from jax import lax
from jax.experimental import pallas as pl
from jax.experimental.pallas import tpu as pltpu
from jax.sharding import PartitionSpec as P


def tables(count):
    modes = jnp.arange(count, dtype=jnp.int32)
    product = modes[:, None] * modes[None, :] % count
    angle = 2.0 * math.pi * product.astype(jnp.float32) / count
    return (jnp.cos(angle), jnp.sin(angle))


def wave_square(index, count):
    freq = jnp.where(index < count // 2, index, index - count).astype(jnp.float32)
    return (2.0 * math.pi * freq / count) ** 2


def contract(form, values, table):
    return jnp.einsum(form, values, table, precision=lax.Precision.HIGHEST)


def rotate(spectrum, form, count, forward):
    cosine, sine = tables(count)
    real_part, imag_part = (spectrum[0], spectrum[1])
    real_cos = contract(form, real_part, cosine)
    real_sin = contract(form, real_part, sine)
    imag_cos = contract(form, imag_part, cosine)
    imag_sin = contract(form, imag_part, sine)
    if forward:
        return jnp.stack([real_cos + imag_sin, imag_cos - real_sin])
    return jnp.stack([real_cos - imag_sin, imag_cos + real_sin])


def per_device_general(concentration, mobility, kappa, well_depth):
    local_species, rows_x, rows_y, depth = concentration.shape
    count_sp = lax.axis_size("sp")
    count_py = lax.axis_size("py")
    count_pz = lax.axis_size("pz")
    full_x = rows_x * count_py
    full_y = rows_y * count_pz
    half_depth = depth // 2
    bulk = well_depth[:, None, None, None] * (
        concentration * concentration * concentration - concentration
    )
    fields = jnp.stack([concentration, bulk])
    cosine, sine = tables(depth)
    alternate = (1 - 2 * (jnp.arange(depth, dtype=jnp.int32) % 2)).astype(jnp.float32)
    spectrum = jnp.stack(
        [
            contract("fsxyz,zk->fsxyk", fields, cosine[:, :half_depth]),
            -contract("fsxyz,zk->fsxyk", fields, sine[:, :half_depth]),
        ]
    )
    spectrum = lax.all_to_all(spectrum, "pz", split_axis=5, concat_axis=4, tiled=True)
    own_lines = spectrum.shape[5]
    highest = contract("fsxyz,z->fsxy", fields, alternate)
    highest = lax.all_gather(highest, "pz", axis=3, tiled=True)
    highest = jnp.stack([highest, jnp.zeros_like(highest)])[..., None]
    spectrum = jnp.concatenate([spectrum, highest], axis=5)
    z_modes = jnp.concatenate(
        [
            lax.axis_index("pz") * own_lines + jnp.arange(own_lines, dtype=jnp.int32),
            jnp.full((1,), half_depth, jnp.int32),
        ]
    )
    spectrum = rotate(spectrum, "fsxyz,yk->fsxkz", full_y, True)
    spectrum = lax.all_to_all(
        lax.all_to_all(spectrum, "sp", split_axis=4, concat_axis=2, tiled=True),
        "py",
        split_axis=4,
        concat_axis=3,
        tiled=True,
    )
    spectrum = rotate(spectrum, "fsxyz,xk->fskyz", full_x, True)
    narrow = spectrum.shape[4]
    lines = spectrum.shape[5]
    y_start = (lax.axis_index("sp") * count_py + lax.axis_index("py")) * narrow
    ksq_x = wave_square(jnp.arange(full_x, dtype=jnp.int32), full_x)
    ksq_y = wave_square(y_start + jnp.arange(narrow, dtype=jnp.int32), full_y)
    ksq_z = wave_square(z_modes, depth)
    ksq = ksq_x[:, None, None] + ksq_y[None, :, None] + ksq_z[None, None, :]
    c_hat = spectrum[:, 0]
    drive = spectrum[:, 1] + kappa[None, :, None, None, None] * ksq[None, None] * c_hat
    mix = jnp.einsum("ij,rjxyz->rixyz", mobility, drive, precision=lax.Precision.HIGHEST)
    stiff = 0.5 * (jnp.diagonal(mobility) * kappa)[:, None, None, None] * (ksq * ksq)[None]
    new_hat = (c_hat * (1.0 + stiff)[None] - 0.5 * ksq[None, None] * mix) / (1.0 + stiff)[None]
    new_hat = rotate(new_hat, "sxyz,xk->skyz", full_x, False)
    moved = lax.all_to_all(
        lax.all_to_all(new_hat, "sp", split_axis=1, concat_axis=3, tiled=True),
        "py",
        split_axis=2,
        concat_axis=3,
        tiled=True,
    )
    moved = moved.reshape(2, local_species, rows_x, count_py, count_sp, narrow, lines)
    moved = moved.transpose(0, 1, 2, 4, 3, 5, 6).reshape(2, local_species, rows_x, full_y, lines)
    moved = rotate(moved, "sxyz,yk->sxkz", full_y, False)
    main = moved[..., : lines - 1]
    highest = moved[0, :, :, :, lines - 1]
    main = lax.all_to_all(main, "pz", split_axis=3, concat_axis=4, tiled=True)
    highest = lax.dynamic_slice_in_dim(highest, lax.axis_index("pz") * rows_y, rows_y, 2)
    weight = jnp.where(jnp.arange(half_depth, dtype=jnp.int32) == 0, 1.0, 2.0).astype(jnp.float32)
    result = contract("sxyk,kz->sxyz", main[0] * weight, cosine[:half_depth]) - contract(
        "sxyk,kz->sxyz", main[1] * weight, sine[:half_depth]
    )
    result = result + highest[..., None] * alternate[None, None, None, :]
    return result * (1.0 / (full_x * full_y * depth))


PIECES = 4
SUBLANES = 8


def basis(count):
    grid = np.arange(count)
    mode = np.arange(count)
    freq = np.minimum(mode, count - mode)
    angle = 2.0 * np.pi * (grid[:, None] * freq[None, :] % count) / count
    table = np.where(mode[None, :] <= count // 2, np.cos(angle), np.sin(angle))
    single = (mode == 0) | (2 * mode == count)
    return table * np.sqrt(np.where(single, 1.0, 2.0) / count)[None, :]


def split_table(table):
    table = table.astype(np.float32)
    high = table.astype(jnp.bfloat16)
    low = (table - high.astype(np.float32)).astype(jnp.bfloat16)
    row = np.concatenate([high, low], axis=1)
    return np.concatenate([row, row], axis=0)


def split(values, axis):
    high = values.astype(jnp.bfloat16)
    low = (values - high.astype(jnp.float32)).astype(jnp.bfloat16)
    return jnp.concatenate([high, low], axis=axis)


def from_right(values, table):
    count = values.shape[1]
    out = jnp.dot(split(values, 1), table, preferred_element_type=jnp.float32)
    return out[:, :count] + out[:, count:]


def from_left(table, values):
    count = table.shape[0] // 2
    out = jnp.dot(table, split(values, 0), preferred_element_type=jnp.float32)
    return out[:count] + out[count:]


def swap_blocks(parts, width):
    parts = list(parts)
    axis = parts[0].ndim - 1
    lanes = parts[0].shape[axis]
    block = lax.broadcasted_iota(jnp.int32, parts[0].shape, axis) // width
    half = len(parts) // 2
    while half:
        low_side = (block // half) % 2 == 0
        for first in range(len(parts)):
            if (first // half) % 2 == 0:
                one, two = parts[first], parts[first + half]
                parts[first] = jnp.where(low_side, one, pltpu.roll(two, half * width, axis))
                parts[first + half] = jnp.where(
                    low_side, pltpu.roll(one, lanes - half * width, axis), two
                )
        half //= 2
    return parts


def kernel(
    sizes, conc_hbm, mobility, kappa, well_depth, right_f_hbm, right_i_hbm, left_f_hbm, left_i_hbm,
    half_f_hbm, half_i_hbm, out,
    conc, right_f, right_i, left_f, left_i, half_f, half_i, own_mix,
    other, depths, other_depths, z_out, z_in, y_out, y_in, near, x_out, x_in, b_out, b_in, w_out, w_in,
    load, table_load, pair_send, pair_recv, depth_send, depth_recv,
    zs, zr, ys, yr, xs, xr, bs, br, ws, wr,
):
    count_py, count_pz = sizes
    species, rows_x, rows_y, n = conc.shape
    me_sp, me_py, me_pz = lax.axis_index("sp"), lax.axis_index("py"), lax.axis_index("pz")
    blocks = count_pz * PIECES
    units = species * PIECES
    width = n // blocks
    groups = rows_x // blocks
    sub = SUBLANES
    strip = rows_x * sub
    mesh_id = pl.DeviceIdType.MESH

    half = me_py // 2
    inner = lax.rem(me_py + half, 2) == 1
    outer = jnp.logical_not(inner)
    buddy = {"sp": me_sp, "py": me_py + 1 - 2 * lax.rem(me_py, 2), "pz": me_pz}
    across = {"sp": me_sp, "py": count_py - 1 - me_py, "pz": me_pz}

    def along_pz(step):
        return {"sp": me_sp, "py": me_py, "pz": lax.rem(me_pz + step, count_pz)}

    partner = {"sp": 1 - me_sp, "py": me_py, "pz": me_pz}
    barrier = pltpu.get_barrier_semaphore()
    peers = [partner, buddy]
    peers += [along_pz(step) for step in range(1, count_pz)]
    for peer in peers:
        pl.semaphore_signal(barrier, inc=1, device_id=peer, device_id_type=mesh_id)

    @pl.when(inner)
    def _():
        pl.semaphore_signal(barrier, inc=1, device_id=across, device_id_type=mesh_id)

    def lot(g):
        return pl.ds(g * blocks, blocks)

    loads = [
        pltpu.make_async_copy(conc_hbm.at[:, lot(g)], conc.at[:, lot(g)], load.at[g])
        for g in range(groups)
    ]
    table_loads = [
        pltpu.make_async_copy(source, target, table_load.at[i])
        for i, (source, target) in enumerate([
            (right_f_hbm, right_f), (left_f_hbm, left_f), (half_f_hbm.at[half], half_f),
            (half_i_hbm.at[half], half_i), (left_i_hbm, left_i), (right_i_hbm, right_i),
        ])
    ]
    for copy in loads + table_loads:
        copy.start()
    for t in range(species):
        depths[t : t + 1, :] = jnp.full((1, n), well_depth[t], jnp.float32)
    for copy in loads:
        copy.wait()
    pl.semaphore_wait(barrier, len(peers) + jnp.where(inner, 1, 0))

    def remote(source, target, send, recv, peer):
        return pltpu.make_async_remote_copy(
            src_ref=source, dst_ref=target, send_sem=send, recv_sem=recv,
            device_id=peer, device_id_type=mesh_id,
        )

    depth_pair = remote(depths, other_depths, depth_send, depth_recv, partner)
    pair = [
        remote(
            conc.at[:, lot(g)], other.at[:, lot(g)], pair_send.at[g], pair_recv.at[g], partner
        )
        for g in range(groups)
    ]
    depth_pair.start()
    for copy in pair:
        copy.start()

    y_rows = pl.ds(pl.multiple_of(me_pz * rows_y, rows_y), rows_y)

    def z_copy(chunk, step, part):
        peer = lax.rem(me_pz + step, count_pz)
        return remote(
            z_out.at[chunk, peer, part], z_in.at[chunk, part, y_rows], zs.at[0],
            zr.at[chunk], along_pz(step),
        )

    def z_all(chunk):
        lines = z_in.at[chunk, :, pl.ds(0, (count_pz - 1) * rows_y)]
        return remote(lines, lines, zs.at[0], zr.at[chunk], partner)

    def y_copy(chunk):
        return remote(y_out.at[chunk], y_in.at[chunk], ys.at[0], yr.at[chunk], buddy)

    near_strip, far_strip = pl.ds(0, strip), pl.ds(strip, strip)

    def x_copy(one, part):
        rows = far_strip if part == 0 else near_strip
        return remote(
            x_out.at[one, rows], x_in.at[one, rows], xs.at[0], xr.at[one, part], across
        )

    def b_copy(one):
        return remote(b_out.at[one], b_in.at[one], bs.at[0], br.at[one], buddy)

    def w_copy(one, step):
        peer = lax.rem(me_pz + step, count_pz)
        return remote(
            w_out.at[one, peer], w_in.at[one, me_pz], ws.at[0], wr.at[one], along_pz(step),
        )

    def w_all(one):
        lines = w_in.at[one, pl.ds(0, count_pz - 1)]
        return remote(lines, lines, ws.at[0], wr.at[one], partner)

    def terms_of(one, side, field, depth):
        own_i = me_sp * species + one
        terms = []
        for t in range(species):
            j = side * species + t
            weight = mobility[own_i, j]
            terms.append((field, t, weight * depth[t : t + 1, :], weight * kappa[j]))
        return terms

    def mixed(terms, x, first=None, second=None):
        for field, t, bulk_weight, conc_weight in terms:
            c = field[t, x]
            a = bulk_weight * (c * c * c - c)
            b = conc_weight * c
            first = a if first is None else first + a
            second = b if second is None else second + b
        return first, second

    def z_forward(one, opening=False):
        own = terms_of(one, me_sp, conc, depths)
        if opening:
            for x in range(rows_x):
                own_mix[0, x], own_mix[1, x] = mixed(own, x)
            depth_pair.wait_recv()
        others = terms_of(one, 1 - me_sp, other, other_depths)
        for g in range(groups):
            if opening:
                pair[g].wait_recv()
            bulk_mix, conc_mix = [], []
            for block in range(blocks):
                x = g * blocks + block
                if opening:
                    first, second = mixed(others, x, own_mix[0, x], own_mix[1, x])
                else:
                    first, second = mixed(own + others, x)
                bulk_mix.append(first)
                conc_mix.append(second)
            modes = from_right(jnp.concatenate(bulk_mix + conc_mix, axis=0), right_f[...])
            modes = modes.reshape(2, blocks, rows_y, n)
            for f in range(2):
                swapped = swap_blocks([modes[f, block] for block in range(blocks)], width)
                for block in range(blocks):
                    unit = PIECES * one + block % PIECES
                    z_out[2 * unit + f, block // PIECES, g] = swapped[block]
            if opening:
                for c in range(2):
                    for step in range(1, count_pz):
                        z_copy(c, step, pl.ds(g, 1)).start()
        for c in range(2 if opening else 0, 2 * PIECES):
            for step in range(1, count_pz):
                z_copy(2 * PIECES * one + c, step, pl.ds(0, groups)).start()
        for c in range(2 * PIECES):
            chunk = 2 * PIECES * one + c
            z_in[chunk, :, y_rows] = z_out[chunk, me_pz]

    def y_chunk(chunk, _):
        z_all(chunk).wait_recv()
        for g in range(0, groups, 2):
            lines = jnp.concatenate([z_in[chunk, g], z_in[chunk, g + 1]], axis=1)
            modes = from_left(left_f[...], lines)
            for h in range(2):
                part = modes[:, h * n : (h + 1) * n].reshape(blocks, sub, n)
                swapped = swap_blocks([part[b] for b in range(blocks)], width)
                for block in range(blocks):
                    start = ((g + h) * blocks + block) * sub
                    y_out[chunk, start : start + sub, :] = swapped[block]

        @pl.when(outer)
        def _():
            y_copy(chunk).start()

        return 0

    def y_forward(one):
        lax.fori_loop(2 * one, 2 * one + 2, y_chunk, 0)

    def square(index):
        freq = jnp.minimum(index, n - index).astype(jnp.float32)
        root = freq * (2.0 * math.pi / n)
        return root * root

    lane = lax.broadcasted_iota(jnp.int32, (1, n), 1)
    ksq_x = square(lax.broadcasted_iota(jnp.int32, (n, 1), 0))

    def x_both(one):
        for f in range(2):
            y_copy(2 * one + f).wait_recv()
        own_i = me_sp * species + one // PIECES
        piece = me_pz * PIECES + lax.rem(one, PIECES)
        ksq_z = square(piece * width + lane % width)
        half_stiff = 0.5 * (mobility[own_i, own_i] * kappa[own_i])
        for r in range(0, sub, 2):
            both, ksq = [], []
            for f in range(2):
                chunk = 2 * one + f
                both.append(from_left(half_f[...], jnp.concatenate([
                    jnp.concatenate([
                        field[chunk, pl.ds(r + h, rows_x, stride=sub), :]
                        for field in (y_out, y_in)
                    ], axis=0)
                    for h in range(2)
                ], axis=1)))
            for h in range(2):
                ksq_y = square((lane // width) * sub + (r + h))
                ksq.append(ksq_x + (ksq_y + ksq_z))
            ksq = jnp.concatenate(ksq, axis=1)
            drop = 0.5 * ksq * (both[0] + ksq * both[1]) / (1.0 + half_stiff * (ksq * ksq))
            lines = from_left(half_i[...], drop)
            for h in range(2):
                rows = pl.ds(r + h, n // 2, stride=sub)
                near[one, rows, :] = lines[: n // 2, h * n : (h + 1) * n]
                x_out[one, rows, :] = lines[n // 2 :, h * n : (h + 1) * n]
        for part in range(2):
            x_copy(one, part).start()

    def combine(one):
        x_copy(one, 0).wait_recv()
        b_out[one] = near[one, strip:, :] + x_in[one, strip:, :]
        b_copy(one).start()
        x_copy(one, 1).wait_recv()
        b_in[one] = near[one, :strip, :] + x_in[one, :strip, :]

    def y_back(one):
        @pl.when(outer)
        def _():
            b_copy(one).wait_recv()

        for g in range(0, groups, 2):
            pairs = []
            for h in range(2):
                parts = []
                for block in range(blocks):
                    start = ((g + h) * blocks + block) * sub
                    parts.append(b_in[one, start : start + sub, :])
                swapped = swap_blocks(parts, width)
                pairs.append(jnp.stack(swapped, axis=0).reshape(n, n))
            lines = from_left(left_i[...], jnp.concatenate(pairs, axis=1))
            for h in range(2):
                part = lines[:, h * n : (h + 1) * n].reshape(count_pz, rows_y, n)
                w_out[one, :, g + h] = part
        for step in range(1, count_pz):
            w_copy(one, step).start()
        w_in[one, me_pz] = w_out[one, me_pz]

    def z_back(one):
        for c in range(PIECES):
            w_all(PIECES * one + c).wait_recv()
        for g in range(0, groups, 2):
            rows = []
            for h in range(2):
                rows += swap_blocks([
                    w_in[PIECES * one + block % PIECES, block // PIECES, g + h]
                    for block in range(blocks)
                ], width)
            lines = from_right(jnp.concatenate(rows, axis=0), right_i[...])
            lines = lines.reshape(2, blocks, rows_y, n)
            for h in range(2):
                for block in range(blocks):
                    x = (g + h) * blocks + block
                    out[one, x] = conc[one, x] - lines[h, block]

    table_loads[0].wait()
    z_forward(0, True)
    for copy in table_loads[1:]:
        copy.wait()
    z_forward(1)
    y_forward(0)
    y_forward(1)
    z_forward(2)
    lag = 2

    def middle(k, _):
        @pl.when(jnp.logical_and(inner, k < units))
        def _():
            x_both(k)

        @pl.when(k == 1)
        def _():
            z_forward(3)

        for ahead in range(2):
            later = 2 * k + 2 + ahead

            @pl.when(later < units)
            def _():
                y_forward(later)

        back = k - lag

        @pl.when(jnp.logical_and(inner, jnp.logical_and(back >= 0, back < units)))
        def _():
            combine(back)

        @pl.when(jnp.logical_and(back >= 0, back < units))
        def _():
            y_back(back)

        done = back - 1
        whole = jnp.logical_and(done > 0, lax.rem(done, PIECES) == 0)

        @pl.when(whole)
        def _():
            z_back(done // PIECES - 1)

        return 0

    lax.fori_loop(0, units + lag + 2, middle, 0)

    depth_pair.wait_send()
    for copy in pair:
        copy.wait_send()
    sent = z_out.at[:, pl.ds(0, count_pz - 1)]
    remote(sent, sent, zs.at[0], zr.at[0], partner).wait_send()
    sent = w_out.at[:, pl.ds(0, count_pz - 1)]
    remote(sent, sent, ws.at[0], wr.at[0], partner).wait_send()

    @pl.when(outer)
    def _():
        remote(y_out, y_in, ys.at[0], yr.at[0], buddy).wait_send()

    @pl.when(inner)
    def _():
        remote(x_out, x_in, xs.at[0], xr.at[0, 0], across).wait_send()
        remote(b_out, b_in, bs.at[0], br.at[0], buddy).wait_send()


def per_device_kernel(concentration, mobility, kappa, well_depth):
    species, rows_x, rows_y, n = concentration.shape
    count_py, count_pz = lax.axis_size("py"), lax.axis_size("pz")
    table = basis(n)
    forward = split_table(table)
    inverse = split_table(table.T)
    blocks = np.arange(n).reshape(count_py, rows_x)
    orders = [blocks[[1, 0, 2, 3]].reshape(n), blocks[[2, 3, 1, 0]].reshape(n)]
    half_forward = np.stack([split_table(table[order[: n // 2]]).T for order in orders])
    half_inverse = np.stack([split_table(table[order].T).T for order in orders])
    blocks = count_pz * PIECES
    units = species * PIECES
    groups = rows_x // blocks
    strip = rows_x * SUBLANES
    f32, bf16 = jnp.float32, jnp.bfloat16
    vmem = pl.BlockSpec(memory_space=pltpu.VMEM)
    smem = pl.BlockSpec(memory_space=pltpu.SMEM)
    hbm = pl.BlockSpec(memory_space=pltpu.HBM)
    dma = pltpu.SemaphoreType.DMA

    def far(array):
        return pltpu.with_memory_space_constraint(array, pltpu.HBM)

    return pl.pallas_call(
        functools.partial(kernel, (count_py, count_pz)),
        out_shape=jax.ShapeDtypeStruct(concentration.shape, f32),
        in_specs=[hbm, smem, smem, smem] + [hbm] * 6,
        out_specs=vmem,
        scratch_shapes=[
            pltpu.VMEM((species, rows_x, rows_y, n), f32),
            pltpu.VMEM(forward.shape, bf16),
            pltpu.VMEM(inverse.shape, bf16),
            pltpu.VMEM(forward.T.shape, bf16),
            pltpu.VMEM(inverse.T.shape, bf16),
            pltpu.VMEM(half_forward.shape[1:], bf16),
            pltpu.VMEM(half_inverse.shape[1:], bf16),
            pltpu.VMEM((2, rows_x, rows_y, n), f32),
            pltpu.VMEM((species, rows_x, rows_y, n), f32),
            pltpu.VMEM((species, n), f32),
            pltpu.VMEM((species, n), f32),
            pltpu.VMEM((2 * units, count_pz, groups, rows_y, n), f32),
            pltpu.VMEM((2 * units, groups, n, n), f32),
            pltpu.VMEM((2 * units, strip, n), f32),
            pltpu.VMEM((2 * units, strip, n), f32),
            pltpu.VMEM((units, 2 * strip, n), f32),
            pltpu.VMEM((units, 2 * strip, n), f32),
            pltpu.VMEM((units, 2 * strip, n), f32),
            pltpu.VMEM((units, strip, n), f32),
            pltpu.VMEM((units, strip, n), f32),
            pltpu.VMEM((units, count_pz, groups, rows_y, n), f32),
            pltpu.VMEM((units, count_pz, groups, rows_y, n), f32),
            dma((groups,)), dma((6,)),
            dma((groups,)), dma((groups,)), dma, dma,
            dma((1,)), dma((2 * units,)),
            dma((1,)), dma((2 * units,)),
            dma((1,)), dma((units, 2)),
            dma((1,)), dma((units,)),
            dma((1,)), dma((units,)),
        ],
        compiler_params=pltpu.CompilerParams(
            collective_id=0, has_side_effects=True, vmem_limit_bytes=46 * 1024 * 1024
        ),
        name="step",
    )(
        far(concentration), far(mobility), far(kappa), far(well_depth),
        *(far(jnp.asarray(each)) for each in (
            forward, inverse, forward.T, inverse.T, half_forward, half_inverse
        )),
    )


def per_device(concentration, mobility, kappa, well_depth):
    species, rows_x, rows_y, n = concentration.shape
    count_sp, count_py, count_pz = (lax.axis_size(name) for name in ("sp", "py", "pz"))
    cube = rows_x * count_py == n and rows_y * count_pz == n and n == 128
    power = count_pz > 1 and count_pz & (count_pz - 1) == 0
    blocks = count_pz * PIECES
    whole = n == SUBLANES * blocks and rows_x % (2 * blocks) == 0 and rows_y % SUBLANES == 0
    if cube and power and whole and count_sp == 2 and count_py == 4 and species == 4:
        return per_device_kernel(concentration, mobility, kappa, well_depth)
    return per_device_general(concentration, mobility, kappa, well_depth)


def solution(mesh):
    in_specs = (P("sp", "py", "pz", None), P(), P(), P("sp"))
    out_specs = P("sp", "py", "pz", None)
    return jax.shard_map(
        per_device, mesh=mesh, in_specs=in_specs, out_specs=out_specs, check_vma=False
    )
```

```python
import functools
import math

import jax
import jax.numpy as jnp
import numpy as np
from jax import lax
from jax.experimental import pallas as pl
from jax.experimental.pallas import tpu as pltpu
from jax.sharding import PartitionSpec as P


def tables(count):
    modes = jnp.arange(count, dtype=jnp.int32)
    product = modes[:, None] * modes[None, :] % count
    angle = 2.0 * math.pi * product.astype(jnp.float32) / count
    return (jnp.cos(angle), jnp.sin(angle))


def wave_square(index, count):
    freq = jnp.where(index < count // 2, index, index - count).astype(jnp.float32)
    return (2.0 * math.pi * freq / count) ** 2


def contract(form, values, table):
    return jnp.einsum(form, values, table, precision=lax.Precision.HIGHEST)


def rotate(spectrum, form, count, forward):
    cosine, sine = tables(count)
    real_part, imag_part = (spectrum[0], spectrum[1])
    real_cos = contract(form, real_part, cosine)
    real_sin = contract(form, real_part, sine)
    imag_cos = contract(form, imag_part, cosine)
    imag_sin = contract(form, imag_part, sine)
    if forward:
        return jnp.stack([real_cos + imag_sin, imag_cos - real_sin])
    return jnp.stack([real_cos - imag_sin, imag_cos + real_sin])


def per_device_general(concentration, mobility, kappa, well_depth):
    local_species, rows_x, rows_y, depth = concentration.shape
    count_sp = lax.axis_size("sp")
    count_py = lax.axis_size("py")
    count_pz = lax.axis_size("pz")
    full_x = rows_x * count_py
    full_y = rows_y * count_pz
    half_depth = depth // 2
    bulk = well_depth[:, None, None, None] * (
        concentration * concentration * concentration - concentration
    )
    fields = jnp.stack([concentration, bulk])
    cosine, sine = tables(depth)
    alternate = (1 - 2 * (jnp.arange(depth, dtype=jnp.int32) % 2)).astype(jnp.float32)
    spectrum = jnp.stack(
        [
            contract("fsxyz,zk->fsxyk", fields, cosine[:, :half_depth]),
            -contract("fsxyz,zk->fsxyk", fields, sine[:, :half_depth]),
        ]
    )
    spectrum = lax.all_to_all(spectrum, "pz", split_axis=5, concat_axis=4, tiled=True)
    own_lines = spectrum.shape[5]
    highest = contract("fsxyz,z->fsxy", fields, alternate)
    highest = lax.all_gather(highest, "pz", axis=3, tiled=True)
    highest = jnp.stack([highest, jnp.zeros_like(highest)])[..., None]
    spectrum = jnp.concatenate([spectrum, highest], axis=5)
    z_modes = jnp.concatenate(
        [
            lax.axis_index("pz") * own_lines + jnp.arange(own_lines, dtype=jnp.int32),
            jnp.full((1,), half_depth, jnp.int32),
        ]
    )
    spectrum = rotate(spectrum, "fsxyz,yk->fsxkz", full_y, True)
    spectrum = lax.all_to_all(
        lax.all_to_all(spectrum, "sp", split_axis=4, concat_axis=2, tiled=True),
        "py",
        split_axis=4,
        concat_axis=3,
        tiled=True,
    )
    spectrum = rotate(spectrum, "fsxyz,xk->fskyz", full_x, True)
    narrow = spectrum.shape[4]
    lines = spectrum.shape[5]
    y_start = (lax.axis_index("sp") * count_py + lax.axis_index("py")) * narrow
    ksq_x = wave_square(jnp.arange(full_x, dtype=jnp.int32), full_x)
    ksq_y = wave_square(y_start + jnp.arange(narrow, dtype=jnp.int32), full_y)
    ksq_z = wave_square(z_modes, depth)
    ksq = ksq_x[:, None, None] + ksq_y[None, :, None] + ksq_z[None, None, :]
    c_hat = spectrum[:, 0]
    drive = spectrum[:, 1] + kappa[None, :, None, None, None] * ksq[None, None] * c_hat
    mix = jnp.einsum("ij,rjxyz->rixyz", mobility, drive, precision=lax.Precision.HIGHEST)
    stiff = 0.5 * (jnp.diagonal(mobility) * kappa)[:, None, None, None] * (ksq * ksq)[None]
    new_hat = (c_hat * (1.0 + stiff)[None] - 0.5 * ksq[None, None] * mix) / (1.0 + stiff)[None]
    new_hat = rotate(new_hat, "sxyz,xk->skyz", full_x, False)
    moved = lax.all_to_all(
        lax.all_to_all(new_hat, "sp", split_axis=1, concat_axis=3, tiled=True),
        "py",
        split_axis=2,
        concat_axis=3,
        tiled=True,
    )
    moved = moved.reshape(2, local_species, rows_x, count_py, count_sp, narrow, lines)
    moved = moved.transpose(0, 1, 2, 4, 3, 5, 6).reshape(2, local_species, rows_x, full_y, lines)
    moved = rotate(moved, "sxyz,yk->sxkz", full_y, False)
    main = moved[..., : lines - 1]
    highest = moved[0, :, :, :, lines - 1]
    main = lax.all_to_all(main, "pz", split_axis=3, concat_axis=4, tiled=True)
    highest = lax.dynamic_slice_in_dim(highest, lax.axis_index("pz") * rows_y, rows_y, 2)
    weight = jnp.where(jnp.arange(half_depth, dtype=jnp.int32) == 0, 1.0, 2.0).astype(jnp.float32)
    result = contract("sxyk,kz->sxyz", main[0] * weight, cosine[:half_depth]) - contract(
        "sxyk,kz->sxyz", main[1] * weight, sine[:half_depth]
    )
    result = result + highest[..., None] * alternate[None, None, None, :]
    return result * (1.0 / (full_x * full_y * depth))


PIECES = 4
SUBLANES = 8
SLOTS = 6


def basis(count):
    grid = np.arange(count)
    mode = np.arange(count)
    freq = np.minimum(mode, count - mode)
    angle = 2.0 * np.pi * (grid[:, None] * freq[None, :] % count) / count
    table = np.where(mode[None, :] <= count // 2, np.cos(angle), np.sin(angle))
    single = (mode == 0) | (2 * mode == count)
    return table * np.sqrt(np.where(single, 1.0, 2.0) / count)[None, :]


def split_table(table):
    table = table.astype(np.float32)
    high = table.astype(jnp.bfloat16)
    low = (table - high.astype(np.float32)).astype(jnp.bfloat16)
    row = np.concatenate([high, low], axis=1)
    return np.concatenate([row, row], axis=0)


def split(values, axis):
    high = values.astype(jnp.bfloat16)
    low = (values - high.astype(jnp.float32)).astype(jnp.bfloat16)
    return jnp.concatenate([high, low], axis=axis)


def from_right(values, table):
    count = values.shape[1]
    out = jnp.dot(split(values, 1), table, preferred_element_type=jnp.float32)
    return out[:, :count] + out[:, count:]


def from_left(table, values):
    count = table.shape[0] // 2
    out = jnp.dot(table, split(values, 0), preferred_element_type=jnp.float32)
    return out[:count] + out[count:]


def swap_blocks(parts, width):
    parts = list(parts)
    axis = parts[0].ndim - 1
    lanes = parts[0].shape[axis]
    block = lax.broadcasted_iota(jnp.int32, parts[0].shape, axis) // width
    half = len(parts) // 2
    while half:
        low_side = (block // half) % 2 == 0
        for first in range(len(parts)):
            if (first // half) % 2 == 0:
                one, two = parts[first], parts[first + half]
                parts[first] = jnp.where(low_side, one, pltpu.roll(two, half * width, axis))
                parts[first + half] = jnp.where(
                    low_side, pltpu.roll(one, lanes - half * width, axis), two
                )
        half //= 2
    return parts


def kernel(
    conc_hbm, mobility_hbm, kappa_hbm, well_depth_hbm, square_hbm, half_f_hbm, half_i_hbm, out,
    mobility, kappa, well_depth, conc, square_tables, half_f, half_i, own_mix,
    other, depths, other_depths, z_out, z_in, y_out, y_in, near, x_out, x_in, b_out, b_in, w_out, w_in,
    load, pair_sent, pair_got, sent, zr, yr, xr, br, wr,
):
    species, rows_x, rows_y, n = conc.shape
    me_sp, me_py, me_pz = lax.axis_index("sp"), lax.axis_index("py"), lax.axis_index("pz")
    count_pz = n // rows_y
    blocks = count_pz * PIECES
    units = species * PIECES
    last = units - 1
    width = n // blocks
    groups = rows_x // blocks
    sub = SUBLANES
    quarters = sub // 2
    mesh_id = pl.DeviceIdType.MESH

    half = me_py // 2
    inner = lax.rem(me_py + half, 2) == 1
    outer = jnp.logical_not(inner)
    buddy = {"sp": me_sp, "py": me_py + 1 - 2 * lax.rem(me_py, 2), "pz": me_pz}
    across = {"sp": me_sp, "py": 3 - me_py, "pz": me_pz}
    partner = {"sp": 1 - me_sp, "py": me_py, "pz": me_pz}
    others_pz = [3 - me_pz, me_pz + 1 - 2 * lax.rem(me_pz, 2), lax.rem(me_pz + 2, 4)]

    def along_pz(peer):
        return {"sp": me_sp, "py": me_py, "pz": peer}

    barrier = pltpu.get_barrier_semaphore()
    peers = [partner, buddy] + [along_pz(peer) for peer in others_pz]
    for peer in peers:
        pl.semaphore_signal(barrier, inc=1, device_id=peer, device_id_type=mesh_id)

    @pl.when(inner)
    def _():
        pl.semaphore_signal(barrier, inc=1, device_id=across, device_id_type=mesh_id)

    def lot(g):
        return pl.ds(g * blocks, blocks)

    moves = [(conc_hbm.at[:, lot(g)], conc.at[:, lot(g)]) for g in range(groups)]
    moves += [
        (well_depth_hbm, well_depth), (mobility_hbm, mobility), (kappa_hbm, kappa),
        (square_hbm, square_tables), (half_f_hbm.at[half], half_f), (half_i_hbm.at[half], half_i),
    ]
    loads = [
        pltpu.make_async_copy(source, target, load.at[i])
        for i, (source, target) in enumerate(moves)
    ]
    for copy in loads:
        copy.start()
    conc_loads, small_loads, table_loads = loads[:groups], loads[groups:-3], loads[-3:]
    right_f, left_f, left_i, right_i = (square_tables.at[i] for i in range(4))
    for copy in small_loads:
        copy.wait()
    for t in range(species):
        depths[t : t + 1, :] = jnp.full((1, n), well_depth[t], jnp.float32)
    pl.semaphore_wait(barrier, len(peers) + jnp.where(inner, 1, 0))

    def remote(source, target, send, recv, peer):
        return pltpu.make_async_remote_copy(
            src_ref=source, dst_ref=target, send_sem=send, recv_sem=recv,
            device_id=peer, device_id_type=mesh_id,
        )

    def waiter(lines, sem):
        return pltpu.make_async_remote_copy(
            src_ref=lines, dst_ref=lines, send_sem=sem, recv_sem=sem,
            device_id=partner, device_id_type=mesh_id,
        )

    depth_pair = remote(depths, other_depths, pair_sent.at[1], pair_got.at[groups], partner)
    pair = [
        remote(
            conc.at[:, lot(g)], other.at[:, lot(g)], pair_sent.at[0], pair_got.at[g], partner
        )
        for g in range(groups)
    ]
    for g in range(groups):
        conc_loads[g].wait()
        pair[g].start()
        if g == 0:
            depth_pair.start()

    y_rows = pl.ds(pl.multiple_of(me_pz * rows_y, rows_y), rows_y)
    z_sent, y_sent, x_sent, b_sent, w_sent = (sent.at[i] for i in range(5))

    def z_copy(chunk, peer, part):
        slot = chunk if chunk < 2 else chunk // 2 + 1
        return remote(
            z_out.at[chunk, peer, part], z_in.at[chunk, part, y_rows], z_sent,
            zr.at[slot], along_pz(peer),
        )

    def z_all(first, count, slot):
        lines = z_in.at[pl.ds(first, count), :, pl.ds(0, (count_pz - 1) * rows_y)]
        return waiter(lines, zr.at[slot])

    def rows_of(q):
        return pl.ds(pl.multiple_of(2 * rows_x * q, 2 * rows_x), 2 * rows_x)

    def slot_of(one):
        return lax.rem(one, SLOTS)

    def y_copy(one, f, q):
        chunk, rows = 2 * one + f, rows_of(q)
        return remote(
            y_out.at[chunk, rows], y_in.at[chunk, rows], y_sent, yr.at[slot_of(one), q], buddy
        )

    def y_all(one, q):
        return waiter(y_in.at[pl.ds(2 * one, 2), rows_of(q)], yr.at[slot_of(one), q])

    def x_copy(one, part, q):
        rows = rows_of(q)
        got = 2 * slot_of(one) + part
        if part:
            got = got + one // last * (2 * SLOTS + q - got)
        return remote(
            x_out.at[one, part, rows], x_in.at[one, part, rows], x_sent, xr.at[got], across
        )

    def x_all(one, part):
        return waiter(x_in.at[one, part], xr.at[2 * slot_of(one) + part])

    def b_all(one):
        return waiter(b_in.at[one], br.at[slot_of(one)])

    def w_copy(one, peer):
        return remote(
            w_out.at[one, peer], w_in.at[one, me_pz], w_sent, wr.at[one // PIECES], along_pz(peer)
        )

    def w_all(one):
        lines = w_in.at[pl.ds(PIECES * one, PIECES), pl.ds(0, count_pz - 1)]
        return waiter(lines, wr.at[one])

    def terms_of(one, side, field, depth):
        own_i = me_sp * species + one
        terms = []
        for t in range(species):
            j = side * species + t
            weight = mobility[own_i, j]
            terms.append((field, t, weight * depth[t : t + 1, :], weight * kappa[j]))
        return terms

    def mixed(terms, x, first=None, second=None):
        for field, t, bulk_weight, conc_weight in terms:
            c = field[t, x]
            a = bulk_weight * (c * c * c - c)
            b = conc_weight * c
            first = a if first is None else first + a
            second = b if second is None else second + b
        return first, second

    def z_part(one, g, opening=False):
        own = terms_of(one, me_sp, conc, depths)
        if opening and g == 0:
            for x in range(rows_x):
                own_mix[0, x], own_mix[1, x] = mixed(own, x)
            depth_pair.wait_recv()
        others = terms_of(one, 1 - me_sp, other, other_depths)
        if opening:
            pair[g].wait_recv()
        bulk_mix, conc_mix = [], []
        for block in range(blocks):
            x = g * blocks + block
            if opening:
                first, second = mixed(others, x, own_mix[0, x], own_mix[1, x])
            else:
                first, second = mixed(own + others, x)
            bulk_mix.append(first)
            conc_mix.append(second)
        modes = from_right(jnp.concatenate(bulk_mix + conc_mix, axis=0), right_f[...])
        modes = modes.reshape(2, blocks, rows_y, n)
        for f in range(2):
            swapped = swap_blocks([modes[f, block] for block in range(blocks)], width)
            for block in range(blocks):
                unit = PIECES * one + block % PIECES
                z_out[2 * unit + f, block // PIECES, g] = swapped[block]
        if opening:
            for c in range(2):
                for peer in others_pz:
                    z_copy(c, peer, pl.ds(g, 1)).start()
        if g == groups - 1:
            for c in range(2 if opening else 0, 2 * PIECES):
                for peer in others_pz:
                    z_copy(2 * PIECES * one + c, peer, pl.ds(0, groups)).start()
            for c in range(2 * PIECES):
                chunk = 2 * PIECES * one + c
                z_in[chunk, :, y_rows] = z_out[chunk, me_pz]

    def y_chunk(chunk):
        for g in range(0, groups, 2):
            lines = jnp.concatenate([z_in[chunk, g], z_in[chunk, g + 1]], axis=1)
            modes = from_left(left_f[...], lines)
            for h in range(2):
                part = modes[:, h * n : (h + 1) * n].reshape(blocks, sub, n)
                swapped = swap_blocks([part[b] for b in range(blocks)], width)
                for block in range(blocks):
                    x = (g + h) * blocks + block
                    y_out[chunk, pl.ds(x, sub, stride=rows_x), :] = swapped[block]

    def y_send(one):
        @pl.when(outer)
        def _():
            for q in range(quarters):
                for f in range(2):
                    y_copy(one, f, q).start()

    def square(index):
        freq = jnp.minimum(index, n - index).astype(jnp.float32)
        root = freq * (2.0 * math.pi / n)
        return root * root

    lane = lax.broadcasted_iota(jnp.int32, (1, n), 1)
    ksq_x = square(lax.broadcasted_iota(jnp.int32, (n, 1), 0))

    def x_quarter(one, q):
        y_all(one, q).wait_recv()
        own_i = me_sp * species + one // PIECES
        piece = me_pz * PIECES + lax.rem(one, PIECES)
        ksq_z = square(piece * width + lane % width)
        half_stiff = 0.5 * (mobility[own_i, own_i] * kappa[own_i])

        def line_rows(h):
            return pl.ds(pl.multiple_of((2 * q + h) * rows_x, rows_x), rows_x)

        both, ksq = [], []
        for f in range(2):
            chunk = 2 * one + f
            both.append(from_left(half_f[...], jnp.concatenate([
                jnp.concatenate([
                    field[chunk, line_rows(h), :] for field in (y_out, y_in)
                ], axis=0)
                for h in range(2)
            ], axis=1)))
        for h in range(2):
            ksq_y = square((lane // width) * sub + (2 * q + h))
            ksq.append(ksq_x + (ksq_y + ksq_z))
        ksq = jnp.concatenate(ksq, axis=1)
        drop = 0.5 * ksq * (both[0] + ksq * both[1]) / (1.0 + half_stiff * (ksq * ksq))
        lines = from_left(half_i[...], drop)
        for h in range(2):
            for i, (field, part) in enumerate([(near, 0), (near, 1), (x_out, 0), (x_out, 1)]):
                field[one, part, line_rows(h), :] = lines[
                    i * rows_x : (i + 1) * rows_x, h * n : (h + 1) * n
                ]
        x_copy(one, 1, q).start()
        x_copy(one, 0, q).start()

    def combine_outer(one):
        x_all(one, 1).wait_recv()
        b_out[one] = near[one, 1] + x_in[one, 1]
        remote(b_out.at[one], b_in.at[one], b_sent, br.at[slot_of(one)], buddy).start()

    def combine_inner(one):
        x_all(one, 0).wait_recv()
        b_in[one] = near[one, 0] + x_in[one, 0]

    def y_back(one):
        for g in range(0, groups, 2):
            pairs = []
            for h in range(2):
                parts = []
                for block in range(blocks):
                    x = (g + h) * blocks + block
                    parts.append(b_in[one, pl.ds(x, sub, stride=rows_x), :])
                swapped = swap_blocks(parts, width)
                pairs.append(jnp.stack(swapped, axis=0).reshape(n, n))
            lines = from_left(left_i[...], jnp.concatenate(pairs, axis=1))
            for h in range(2):
                part = lines[:, h * n : (h + 1) * n].reshape(count_pz, rows_y, n)
                w_out[one, :, g + h] = part
        for peer in others_pz:
            w_copy(one, peer).start()
        w_in[one, me_pz] = w_out[one, me_pz]

    def back(one):
        @pl.when(inner)
        def _():
            combine_inner(one)

        @pl.when(outer)
        def _():
            b_all(one).wait_recv()

        y_back(one)

    def z_back(one):
        w_all(one).wait_recv()
        for g in range(0, groups, 2):
            rows = []
            for h in range(2):
                rows += swap_blocks([
                    w_in[PIECES * one + block % PIECES, block // PIECES, g + h]
                    for block in range(blocks)
                ], width)
            lines = from_right(jnp.concatenate(rows, axis=0), right_i[...])
            lines = lines.reshape(2, blocks, rows_y, n)
            for h in range(2):
                for block in range(blocks):
                    x = (g + h) * blocks + block
                    out[one, x] = conc[one, x] - lines[h, block]

    table_loads[0].wait()
    for g in range(groups):
        z_part(0, g, True)
    for copy in table_loads[1:]:
        copy.wait()
    for g in range(groups):
        z_part(1, g)
    for f in range(2):
        z_all(f, 1, f).wait_recv()
        y_chunk(f)
    y_send(0)
    z_all(2, 2, 2).wait_recv()
    for f in range(2):
        y_chunk(2 + f)
    y_send(1)
    extra = {}
    for one in range(2, species):
        for g in range(groups):
            extra[1 + (one - 2) * groups + g] = functools.partial(z_part, one, g)
    for one in range(species - 1):
        extra[units - 2 * (species - 1 - one)] = functools.partial(z_back, one)

    def middle(step, _):
        one, q = step // quarters, lax.rem(step, quarters)
        ahead, behind = one + 2, one - 2

        @pl.when(inner)
        def _():
            x_quarter(one, q)

        @pl.when(jnp.logical_and(inner, jnp.logical_and(behind >= 0, q == 0)))
        def _():
            combine_outer(behind)

        @pl.when(jnp.logical_and(ahead < units, q == 0))
        def _():
            z_all(2 * ahead, 2, ahead + 1).wait_recv()

        @pl.when(jnp.logical_and(ahead < units, q < 2))
        def _():
            y_chunk(2 * ahead + q)

        @pl.when(jnp.logical_and(ahead < units, q == 1))
        def _():
            y_send(ahead)

        @pl.when(jnp.logical_and(behind >= 0, q == 2))
        def _():
            back(behind)

        for unit, work in extra.items():
            @pl.when(jnp.logical_and(one == unit, q == 3))
            def _(work=work):
                work()

        return 0

    lax.fori_loop(0, units * quarters, middle, 0)

    @pl.when(inner)
    def _():
        combine_outer(last - 1)

    back(last - 1)

    @pl.when(inner)
    def _():
        for q in range(quarters):
            rows = rows_of(q)
            x_copy(last, 1, q).wait_recv()
            b_out[last, rows, :] = near[last, 1, rows, :] + x_in[last, 1, rows, :]
            remote(
                b_out.at[last, rows], b_in.at[last, rows], b_sent, br.at[last % SLOTS], buddy
            ).start()
        combine_inner(last)

    @pl.when(outer)
    def _():
        b_all(last).wait_recv()

    y_back(last)
    z_back(species - 1)

    depth_pair.wait_send()
    waiter(conc, pair_sent.at[0]).wait_send()
    waiter(z_out.at[:, pl.ds(0, count_pz - 1)], z_sent).wait_send()

    @pl.when(outer)
    def _():
        waiter(y_out, y_sent).wait_send()

    @pl.when(inner)
    def _():
        waiter(x_out, x_sent).wait_send()
        waiter(b_out, b_sent).wait_send()

    waiter(w_out.at[:, pl.ds(0, count_pz - 1)], w_sent).wait_send()


def per_device_kernel(concentration, mobility, kappa, well_depth):
    species, rows_x, rows_y, n = concentration.shape
    count_py, count_pz = lax.axis_size("py"), lax.axis_size("pz")
    table = basis(n)
    forward = split_table(table)
    inverse = split_table(table.T)
    square_tables = np.stack([forward, forward.T, inverse.T, inverse])
    blocks = np.arange(n).reshape(count_py, rows_x)
    orders = [blocks[[1, 0, 2, 3]].reshape(n), blocks[[2, 3, 1, 0]].reshape(n)]
    half_forward = np.stack([split_table(table[order[: n // 2]]).T for order in orders])
    half_inverse = np.stack([split_table(table[order].T).T for order in orders])
    blocks = count_pz * PIECES
    units = species * PIECES
    groups = rows_x // blocks
    strip = rows_x * SUBLANES
    f32, bf16 = jnp.float32, jnp.bfloat16
    hbm = pl.BlockSpec(memory_space=pltpu.HBM)
    dma = pltpu.SemaphoreType.DMA

    def far(array):
        return pltpu.with_memory_space_constraint(array, pltpu.HBM)

    return pl.pallas_call(
        kernel,
        out_shape=jax.ShapeDtypeStruct(concentration.shape, f32),
        in_specs=[hbm] * 7,
        out_specs=pl.BlockSpec(memory_space=pltpu.VMEM),
        scratch_shapes=[
            pltpu.SMEM(mobility.shape, f32),
            pltpu.SMEM(kappa.shape, f32),
            pltpu.SMEM(well_depth.shape, f32),
            pltpu.VMEM((species, rows_x, rows_y, n), f32),
            pltpu.VMEM(square_tables.shape, bf16),
            pltpu.VMEM(half_forward.shape[1:], bf16),
            pltpu.VMEM(half_inverse.shape[1:], bf16),
            pltpu.VMEM((2, rows_x, rows_y, n), f32),
            pltpu.VMEM((species, rows_x, rows_y, n), f32),
            pltpu.VMEM((species, n), f32),
            pltpu.VMEM((species, n), f32),
            pltpu.VMEM((2 * units, count_pz, groups, rows_y, n), f32),
            pltpu.VMEM((2 * units, groups, n, n), f32),
            pltpu.VMEM((2 * units, strip, n), f32),
            pltpu.VMEM((2 * units, strip, n), f32),
            pltpu.VMEM((units, 2, strip, n), f32),
            pltpu.VMEM((units, 2, strip, n), f32),
            pltpu.VMEM((units, 2, strip, n), f32),
            pltpu.VMEM((units, strip, n), f32),
            pltpu.VMEM((units, strip, n), f32),
            pltpu.VMEM((units, count_pz, groups, rows_y, n), f32),
            pltpu.VMEM((units, count_pz, groups, rows_y, n), f32),
            dma((groups + 6,)), dma((2,)), dma((groups + 1,)), dma((5,)),
            dma((units + 1,)), dma((SLOTS, SUBLANES // 2)), dma((2 * SLOTS + 4,)), dma((SLOTS,)),
            dma((species,)),
        ],
        compiler_params=pltpu.CompilerParams(
            collective_id=0, has_side_effects=True, vmem_limit_bytes=46 * 1024 * 1024
        ),
        name="step",
    )(*(
        far(jnp.asarray(each)) for each in (
            concentration, mobility, kappa, well_depth, square_tables, half_forward, half_inverse
        )
    ))


def per_device(concentration, mobility, kappa, well_depth):
    species, rows_x, rows_y, n = concentration.shape
    count_sp, count_py, count_pz = (lax.axis_size(name) for name in ("sp", "py", "pz"))
    cube = rows_x * count_py == n and rows_y * count_pz == n and n == 128
    blocks = count_pz * PIECES
    whole = n == SUBLANES * blocks and rows_x % (2 * blocks) == 0 and rows_y % SUBLANES == 0
    if cube and whole and count_sp == 2 and count_py == 4 and count_pz == 4 and species == 4:
        return per_device_kernel(concentration, mobility, kappa, well_depth)
    return per_device_general(concentration, mobility, kappa, well_depth)


def solution(mesh):
    in_specs = (P("sp", "py", "pz", None), P(), P(), P("sp"))
    out_specs = P("sp", "py", "pz", None)
    return jax.shard_map(
        per_device, mesh=mesh, in_specs=in_specs, out_specs=out_specs, check_vma=False
    )
```

```python
import functools
import math

import jax
import jax.numpy as jnp
import numpy as np
from jax import lax
from jax.experimental import pallas as pl
from jax.experimental.pallas import tpu as pltpu
from jax.sharding import PartitionSpec as P


def tables(count):
    modes = jnp.arange(count, dtype=jnp.int32)
    product = modes[:, None] * modes[None, :] % count
    angle = 2.0 * math.pi * product.astype(jnp.float32) / count
    return (jnp.cos(angle), jnp.sin(angle))


def wave_square(index, count):
    freq = jnp.where(index < count // 2, index, index - count).astype(jnp.float32)
    return (2.0 * math.pi * freq / count) ** 2


def contract(form, values, table):
    return jnp.einsum(form, values, table, precision=lax.Precision.HIGHEST)


def rotate(spectrum, form, count, forward):
    cosine, sine = tables(count)
    real_part, imag_part = (spectrum[0], spectrum[1])
    real_cos = contract(form, real_part, cosine)
    real_sin = contract(form, real_part, sine)
    imag_cos = contract(form, imag_part, cosine)
    imag_sin = contract(form, imag_part, sine)
    if forward:
        return jnp.stack([real_cos + imag_sin, imag_cos - real_sin])
    return jnp.stack([real_cos - imag_sin, imag_cos + real_sin])


def per_device_general(concentration, mobility, kappa, well_depth):
    local_species, rows_x, rows_y, depth = concentration.shape
    count_sp = lax.axis_size("sp")
    count_py = lax.axis_size("py")
    count_pz = lax.axis_size("pz")
    full_x = rows_x * count_py
    full_y = rows_y * count_pz
    half_depth = depth // 2
    bulk = well_depth[:, None, None, None] * (
        concentration * concentration * concentration - concentration
    )
    fields = jnp.stack([concentration, bulk])
    cosine, sine = tables(depth)
    alternate = (1 - 2 * (jnp.arange(depth, dtype=jnp.int32) % 2)).astype(jnp.float32)
    spectrum = jnp.stack(
        [
            contract("fsxyz,zk->fsxyk", fields, cosine[:, :half_depth]),
            -contract("fsxyz,zk->fsxyk", fields, sine[:, :half_depth]),
        ]
    )
    spectrum = lax.all_to_all(spectrum, "pz", split_axis=5, concat_axis=4, tiled=True)
    own_lines = spectrum.shape[5]
    highest = contract("fsxyz,z->fsxy", fields, alternate)
    highest = lax.all_gather(highest, "pz", axis=3, tiled=True)
    highest = jnp.stack([highest, jnp.zeros_like(highest)])[..., None]
    spectrum = jnp.concatenate([spectrum, highest], axis=5)
    z_modes = jnp.concatenate(
        [
            lax.axis_index("pz") * own_lines + jnp.arange(own_lines, dtype=jnp.int32),
            jnp.full((1,), half_depth, jnp.int32),
        ]
    )
    spectrum = rotate(spectrum, "fsxyz,yk->fsxkz", full_y, True)
    spectrum = lax.all_to_all(
        lax.all_to_all(spectrum, "sp", split_axis=4, concat_axis=2, tiled=True),
        "py",
        split_axis=4,
        concat_axis=3,
        tiled=True,
    )
    spectrum = rotate(spectrum, "fsxyz,xk->fskyz", full_x, True)
    narrow = spectrum.shape[4]
    lines = spectrum.shape[5]
    y_start = (lax.axis_index("sp") * count_py + lax.axis_index("py")) * narrow
    ksq_x = wave_square(jnp.arange(full_x, dtype=jnp.int32), full_x)
    ksq_y = wave_square(y_start + jnp.arange(narrow, dtype=jnp.int32), full_y)
    ksq_z = wave_square(z_modes, depth)
    ksq = ksq_x[:, None, None] + ksq_y[None, :, None] + ksq_z[None, None, :]
    c_hat = spectrum[:, 0]
    drive = spectrum[:, 1] + kappa[None, :, None, None, None] * ksq[None, None] * c_hat
    mix = jnp.einsum("ij,rjxyz->rixyz", mobility, drive, precision=lax.Precision.HIGHEST)
    stiff = 0.5 * (jnp.diagonal(mobility) * kappa)[:, None, None, None] * (ksq * ksq)[None]
    new_hat = (c_hat * (1.0 + stiff)[None] - 0.5 * ksq[None, None] * mix) / (1.0 + stiff)[None]
    new_hat = rotate(new_hat, "sxyz,xk->skyz", full_x, False)
    moved = lax.all_to_all(
        lax.all_to_all(new_hat, "sp", split_axis=1, concat_axis=3, tiled=True),
        "py",
        split_axis=2,
        concat_axis=3,
        tiled=True,
    )
    moved = moved.reshape(2, local_species, rows_x, count_py, count_sp, narrow, lines)
    moved = moved.transpose(0, 1, 2, 4, 3, 5, 6).reshape(2, local_species, rows_x, full_y, lines)
    moved = rotate(moved, "sxyz,yk->sxkz", full_y, False)
    main = moved[..., : lines - 1]
    highest = moved[0, :, :, :, lines - 1]
    main = lax.all_to_all(main, "pz", split_axis=3, concat_axis=4, tiled=True)
    highest = lax.dynamic_slice_in_dim(highest, lax.axis_index("pz") * rows_y, rows_y, 2)
    weight = jnp.where(jnp.arange(half_depth, dtype=jnp.int32) == 0, 1.0, 2.0).astype(jnp.float32)
    result = contract("sxyk,kz->sxyz", main[0] * weight, cosine[:half_depth]) - contract(
        "sxyk,kz->sxyz", main[1] * weight, sine[:half_depth]
    )
    result = result + highest[..., None] * alternate[None, None, None, :]
    return result * (1.0 / (full_x * full_y * depth))


PIECES = 4
SUBLANES = 8
SLOTS = 6
STEPS = 16
LAG = 5
DIRECT = 2


def basis(count):
    grid = np.arange(count)
    mode = np.arange(count)
    freq = np.minimum(mode, count - mode)
    angle = 2.0 * np.pi * (grid[:, None] * freq[None, :] % count) / count
    table = np.where(mode[None, :] <= count // 2, np.cos(angle), np.sin(angle))
    single = (mode == 0) | (2 * mode == count)
    return table * np.sqrt(np.where(single, 1.0, 2.0) / count)[None, :]


def split_table(table):
    table = table.astype(np.float32)
    high = table.astype(jnp.bfloat16)
    low = (table - high.astype(np.float32)).astype(jnp.bfloat16)
    row = np.concatenate([high, low], axis=1)
    return np.concatenate([row, row], axis=0)


def split(values, axis):
    high = values.astype(jnp.bfloat16)
    low = (values - high.astype(jnp.float32)).astype(jnp.bfloat16)
    return jnp.concatenate([high, low], axis=axis)


def from_right(values, table):
    count = values.shape[1]
    out = jnp.dot(split(values, 1), table, preferred_element_type=jnp.float32)
    return out[:, :count] + out[:, count:]


def from_left(table, values):
    count = table.shape[0] // 2
    out = jnp.dot(table, split(values, 0), preferred_element_type=jnp.float32)
    return out[:count] + out[count:]


def swap_blocks(parts, width):
    parts = list(parts)
    axis = parts[0].ndim - 1
    lanes = parts[0].shape[axis]
    block = lax.broadcasted_iota(jnp.int32, parts[0].shape, axis) // width
    half = len(parts) // 2
    while half:
        low_side = (block // half) % 2 == 0
        for first in range(len(parts)):
            if (first // half) % 2 == 0:
                one, two = parts[first], parts[first + half]
                parts[first] = jnp.where(low_side, one, pltpu.roll(two, half * width, axis))
                parts[first + half] = jnp.where(
                    low_side, pltpu.roll(one, lanes - half * width, axis), two
                )
        half //= 2
    return parts


def kernel(
    conc_hbm, mobility_hbm, kappa_hbm, well_depth_hbm, square_hbm, half_f_hbm, half_i_hbm, out,
    mobility, kappa, well_depth, conc, square_tables, half_f, half_i, own_mix,
    other, depths, other_depths, z_out, z_in, y_out, y_in, near, x_out, x_in, b_out, b_in, w_out, w_in,
    load, pair_sent, pair_got, sent, zr, yr, xr, br, wr,
):
    species, rows_x, rows_y, n = conc.shape
    me_sp, me_py, me_pz = lax.axis_index("sp"), lax.axis_index("py"), lax.axis_index("pz")
    count_pz = n // rows_y
    blocks = count_pz * PIECES
    units = species * PIECES
    last = units - 1
    width = n // blocks
    groups = rows_x // blocks
    sub = SUBLANES
    quarters = sub // 2
    mesh_id = pl.DeviceIdType.MESH

    half = me_py // 2
    inner = lax.rem(me_py + half, 2) == 1
    outer = jnp.logical_not(inner)
    buddy = {"sp": me_sp, "py": me_py + 1 - 2 * lax.rem(me_py, 2), "pz": me_pz}
    across_py = 3 - me_py
    far_py = lax.rem(me_py + 2, 4)
    across = {"sp": me_sp, "py": across_py, "pz": me_pz}
    partner = {"sp": 1 - me_sp, "py": me_py, "pz": me_pz}
    others_pz = [3 - me_pz, me_pz + 1 - 2 * lax.rem(me_pz, 2), lax.rem(me_pz + 2, 4)]

    def along_pz(peer):
        return {"sp": me_sp, "py": me_py, "pz": peer}

    barrier = pltpu.get_barrier_semaphore()
    peers = [partner, buddy] + [along_pz(peer) for peer in others_pz]
    for peer in peers:
        pl.semaphore_signal(barrier, inc=1, device_id=peer, device_id_type=mesh_id)

    @pl.when(inner)
    def _():
        pl.semaphore_signal(barrier, inc=1, device_id=across, device_id_type=mesh_id)

    def lot(g):
        return pl.ds(g * blocks, blocks)

    moves = [(conc_hbm.at[:, lot(g)], conc.at[:, lot(g)]) for g in range(groups)]
    moves += [
        (well_depth_hbm, well_depth), (mobility_hbm, mobility), (kappa_hbm, kappa),
        (square_hbm, square_tables), (half_f_hbm.at[half], half_f), (half_i_hbm.at[half], half_i),
    ]
    loads = [
        pltpu.make_async_copy(source, target, load.at[i])
        for i, (source, target) in enumerate(moves)
    ]
    for copy in loads:
        copy.start()
    conc_loads, small_loads, table_loads = loads[:groups], loads[groups:-3], loads[-3:]
    right_f, left_f, left_i, right_i = (square_tables.at[i] for i in range(4))
    for copy in small_loads:
        copy.wait()
    for t in range(species):
        depths[t : t + 1, :] = jnp.full((1, n), well_depth[t], jnp.float32)
    pl.semaphore_wait(barrier, len(peers) + jnp.where(inner, 1, 0))

    def remote(source, target, send, recv, peer):
        return pltpu.make_async_remote_copy(
            src_ref=source, dst_ref=target, send_sem=send, recv_sem=recv,
            device_id=peer, device_id_type=mesh_id,
        )

    def waiter(lines, sem):
        return pltpu.make_async_remote_copy(
            src_ref=lines, dst_ref=lines, send_sem=sem, recv_sem=sem,
            device_id=partner, device_id_type=mesh_id,
        )

    depth_pair = remote(depths, other_depths, pair_sent.at[1], pair_got.at[groups], partner)
    pair = [
        remote(
            conc.at[:, lot(g)], other.at[:, lot(g)], pair_sent.at[0], pair_got.at[g], partner
        )
        for g in range(groups)
    ]
    for g in range(groups):
        conc_loads[g].wait()
        pair[g].start()
        if g == 0:
            depth_pair.start()

    y_rows = pl.ds(pl.multiple_of(me_pz * rows_y, rows_y), rows_y)
    z_sent, y_sent, x_sent, b_sent, w_sent = (sent.at[i] for i in range(5))

    def z_copy(chunk, peer, part):
        slot = chunk if chunk < 2 else chunk // 2 + 1
        return remote(
            z_out.at[chunk, peer, part], z_in.at[chunk, part, y_rows], z_sent,
            zr.at[slot], along_pz(peer),
        )

    def z_all(first, count, slot):
        lines = z_in.at[pl.ds(first, count), :, pl.ds(0, (count_pz - 1) * rows_y)]
        return waiter(lines, zr.at[slot])

    def rows_of(q):
        return pl.ds(pl.multiple_of(2 * rows_x * q, 2 * rows_x), 2 * rows_x)

    def slot_of(one):
        return lax.rem(one, SLOTS)

    def y_copy(one, f, q):
        chunk, rows = 2 * one + f, rows_of(q)
        return remote(
            y_out.at[chunk, rows], y_in.at[chunk, rows], y_sent, yr.at[slot_of(one), q], buddy
        )

    def y_all(one, q):
        return waiter(y_in.at[pl.ds(2 * one, 2), rows_of(q)], yr.at[slot_of(one), q])

    def x_copy(one, part, q):
        rows = rows_of(q)
        got = slot_of(one)
        target = across
        if part:
            got = SLOTS + lax.rem(one * quarters + q, STEPS)
            direct = (one * quarters + q) // (units * quarters - DIRECT)
            target = {"sp": me_sp, "py": across_py + direct * (far_py - across_py), "pz": me_pz}
        return remote(
            x_out.at[one, part, rows], x_in.at[one, part, rows], x_sent, xr.at[got], target
        )

    def x_all(one):
        return waiter(x_in.at[one, 0], xr.at[slot_of(one)])

    def b_all(one):
        return waiter(b_in.at[one], br.at[slot_of(one)])

    def w_copy(one, peer):
        return remote(
            w_out.at[one, peer], w_in.at[one, me_pz], w_sent, wr.at[one // PIECES], along_pz(peer)
        )

    def w_all(one):
        lines = w_in.at[pl.ds(PIECES * one, PIECES), pl.ds(0, count_pz - 1)]
        return waiter(lines, wr.at[one])

    def terms_of(one, side, field, depth):
        own_i = me_sp * species + one
        terms = []
        for t in range(species):
            j = side * species + t
            weight = mobility[own_i, j]
            terms.append((field, t, weight * depth[t : t + 1, :], weight * kappa[j]))
        return terms

    def mixed(terms, x, first=None, second=None):
        for field, t, bulk_weight, conc_weight in terms:
            c = field[t, x]
            a = bulk_weight * (c * c * c - c)
            b = conc_weight * c
            first = a if first is None else first + a
            second = b if second is None else second + b
        return first, second

    def z_part(one, g, opening=False):
        own = terms_of(one, me_sp, conc, depths)
        if opening and g == 0:
            for x in range(rows_x):
                own_mix[0, x], own_mix[1, x] = mixed(own, x)
            depth_pair.wait_recv()
        others = terms_of(one, 1 - me_sp, other, other_depths)
        if opening:
            pair[g].wait_recv()
        bulk_mix, conc_mix = [], []
        for block in range(blocks):
            x = g * blocks + block
            if opening:
                first, second = mixed(others, x, own_mix[0, x], own_mix[1, x])
            else:
                first, second = mixed(own + others, x)
            bulk_mix.append(first)
            conc_mix.append(second)
        modes = from_right(jnp.concatenate(bulk_mix + conc_mix, axis=0), right_f[...])
        modes = modes.reshape(2, blocks, rows_y, n)
        for f in range(2):
            swapped = swap_blocks([modes[f, block] for block in range(blocks)], width)
            for block in range(blocks):
                unit = PIECES * one + block % PIECES
                z_out[2 * unit + f, block // PIECES, g] = swapped[block]
        if opening:
            for c in range(2):
                for peer in others_pz:
                    z_copy(c, peer, pl.ds(g, 1)).start()
        if g == groups - 1:
            for c in range(2 if opening else 0, 2 * PIECES):
                for peer in others_pz:
                    z_copy(2 * PIECES * one + c, peer, pl.ds(0, groups)).start()
            for c in range(2 * PIECES):
                chunk = 2 * PIECES * one + c
                z_in[chunk, :, y_rows] = z_out[chunk, me_pz]

    def y_chunk(chunk):
        for g in range(0, groups, 2):
            lines = jnp.concatenate([z_in[chunk, g], z_in[chunk, g + 1]], axis=1)
            modes = from_left(left_f[...], lines)
            for h in range(2):
                part = modes[:, h * n : (h + 1) * n].reshape(blocks, sub, n)
                swapped = swap_blocks([part[b] for b in range(blocks)], width)
                for block in range(blocks):
                    x = (g + h) * blocks + block
                    y_out[chunk, pl.ds(x, sub, stride=rows_x), :] = swapped[block]

    def y_send(one):
        @pl.when(outer)
        def _():
            for q in range(quarters):
                for f in range(2):
                    y_copy(one, f, q).start()

    def square(index):
        freq = jnp.minimum(index, n - index).astype(jnp.float32)
        root = freq * (2.0 * math.pi / n)
        return root * root

    lane = lax.broadcasted_iota(jnp.int32, (1, n), 1)
    ksq_x = square(lax.broadcasted_iota(jnp.int32, (n, 1), 0))

    def x_quarter(one, q):
        y_all(one, q).wait_recv()
        own_i = me_sp * species + one // PIECES
        piece = me_pz * PIECES + lax.rem(one, PIECES)
        ksq_z = square(piece * width + lane % width)
        half_stiff = 0.5 * (mobility[own_i, own_i] * kappa[own_i])

        def line_rows(h):
            return pl.ds(pl.multiple_of((2 * q + h) * rows_x, rows_x), rows_x)

        both, ksq = [], []
        for f in range(2):
            chunk = 2 * one + f
            both.append(from_left(half_f[...], jnp.concatenate([
                jnp.concatenate([
                    field[chunk, line_rows(h), :] for field in (y_out, y_in)
                ], axis=0)
                for h in range(2)
            ], axis=1)))
        for h in range(2):
            ksq_y = square((lane // width) * sub + (2 * q + h))
            ksq.append(ksq_x + (ksq_y + ksq_z))
        ksq = jnp.concatenate(ksq, axis=1)
        drop = 0.5 * ksq * (both[0] + ksq * both[1]) / (1.0 + half_stiff * (ksq * ksq))
        lines = from_left(half_i[...], drop)
        for h in range(2):
            for i, (field, part) in enumerate([(near, 0), (near, 1), (x_out, 0), (x_out, 1)]):
                field[one, part, line_rows(h), :] = lines[
                    i * rows_x : (i + 1) * rows_x, h * n : (h + 1) * n
                ]
        x_copy(one, 1, q).start()
        x_copy(one, 0, q).start()

        @pl.when(one * quarters + q >= units * quarters - DIRECT)
        def _():
            rows = rows_of(q)
            remote(
                near.at[last, 1, rows], b_in.at[last, rows], b_sent, br.at[last % SLOTS], buddy
            ).start()

    def combine_quarter(step):
        one, q = step // quarters, lax.rem(step, quarters)
        rows = rows_of(q)
        x_copy(one, 1, q).wait_recv()
        b_out[one, rows, :] = near[one, 1, rows, :] + x_in[one, 1, rows, :]
        remote(
            b_out.at[one, rows], b_in.at[one, rows], b_sent, br.at[slot_of(one)], buddy
        ).start()

    def combine_inner(one):
        x_all(one).wait_recv()
        b_in[one] = near[one, 0] + x_in[one, 0]

    def y_back(one):
        for g in range(0, groups, 2):
            pairs = []
            for h in range(2):
                parts = []
                for block in range(blocks):
                    x = (g + h) * blocks + block
                    parts.append(b_in[one, pl.ds(x, sub, stride=rows_x), :])
                swapped = swap_blocks(parts, width)
                pairs.append(jnp.stack(swapped, axis=0).reshape(n, n))
            lines = from_left(left_i[...], jnp.concatenate(pairs, axis=1))
            for h in range(2):
                part = lines[:, h * n : (h + 1) * n].reshape(count_pz, rows_y, n)
                w_out[one, :, g + h] = part
        for peer in others_pz:
            w_copy(one, peer).start()
        w_in[one, me_pz] = w_out[one, me_pz]

    def back(one):
        @pl.when(inner)
        def _():
            combine_inner(one)

        @pl.when(outer)
        def _():
            b_all(one).wait_recv()

        y_back(one)

    def z_back(one):
        w_all(one).wait_recv()
        for g in range(0, groups, 2):
            rows = []
            for h in range(2):
                rows += swap_blocks([
                    w_in[PIECES * one + block % PIECES, block // PIECES, g + h]
                    for block in range(blocks)
                ], width)
            lines = from_right(jnp.concatenate(rows, axis=0), right_i[...])
            lines = lines.reshape(2, blocks, rows_y, n)
            for h in range(2):
                for block in range(blocks):
                    x = (g + h) * blocks + block
                    out[one, x] = conc[one, x] - lines[h, block]

    table_loads[0].wait()
    for g in range(groups):
        z_part(0, g, True)
    for copy in table_loads[1:]:
        copy.wait()
    for g in range(groups):
        z_part(1, g)
    for f in range(2):
        z_all(f, 1, f).wait_recv()
        y_chunk(f)
    y_send(0)
    z_all(2, 2, 2).wait_recv()
    for f in range(2):
        y_chunk(2 + f)
    y_send(1)
    extra = {}
    for one in range(2, species):
        for g in range(groups):
            extra[1 + (one - 2) * groups + g] = functools.partial(z_part, one, g)
    for one in range(species - 1):
        extra[units - 2 * (species - 1 - one)] = functools.partial(z_back, one)

    def middle(step, _):
        one, q = step // quarters, lax.rem(step, quarters)
        ahead, behind = one + 2, one - 2

        @pl.when(jnp.logical_and(inner, step >= LAG))
        def _():
            combine_quarter(step - LAG)

        @pl.when(inner)
        def _():
            x_quarter(one, q)

        @pl.when(jnp.logical_and(ahead < units, q == 0))
        def _():
            z_all(2 * ahead, 2, ahead + 1).wait_recv()

        @pl.when(jnp.logical_and(ahead < units, q < 2))
        def _():
            y_chunk(2 * ahead + q)

        @pl.when(jnp.logical_and(ahead < units, q == 1))
        def _():
            y_send(ahead)

        @pl.when(jnp.logical_and(behind >= 0, q == 2))
        def _():
            back(behind)

        for unit, work in extra.items():
            @pl.when(jnp.logical_and(one == unit, q == 3))
            def _(work=work):
                work()

        return 0

    steps = units * quarters
    lax.fori_loop(0, steps, middle, 0)

    def returns(step, _):
        combine_quarter(step)
        return 0

    @pl.when(inner)
    def _():
        lax.fori_loop(steps - LAG, steps - quarters, returns, 0)

    back(last - 1)

    @pl.when(inner)
    def _():
        lax.fori_loop(steps - quarters, steps - DIRECT, returns, 0)
        combine_inner(last)

    @pl.when(outer)
    def _():
        b_all(last).wait_recv()
        for q in range(quarters - DIRECT, quarters):
            x_copy(last, 1, q).wait_recv()
            rows = rows_of(q)
            b_in[last, rows, :] = b_in[last, rows, :] + x_in[last, 1, rows, :]

    y_back(last)
    z_back(species - 1)

    depth_pair.wait_send()
    waiter(conc, pair_sent.at[0]).wait_send()
    waiter(z_out.at[:, pl.ds(0, count_pz - 1)], z_sent).wait_send()

    @pl.when(outer)
    def _():
        waiter(y_out, y_sent).wait_send()

    @pl.when(inner)
    def _():
        waiter(x_out, x_sent).wait_send()
        waiter(b_out, b_sent).wait_send()

    waiter(w_out.at[:, pl.ds(0, count_pz - 1)], w_sent).wait_send()


def per_device_kernel(concentration, mobility, kappa, well_depth):
    species, rows_x, rows_y, n = concentration.shape
    count_py, count_pz = lax.axis_size("py"), lax.axis_size("pz")
    table = basis(n)
    forward = split_table(table)
    inverse = split_table(table.T)
    square_tables = np.stack([forward, forward.T, inverse.T, inverse])
    blocks = np.arange(n).reshape(count_py, rows_x)
    orders = [blocks[[1, 0, 2, 3]].reshape(n), blocks[[2, 3, 1, 0]].reshape(n)]
    half_forward = np.stack([split_table(table[order[: n // 2]]).T for order in orders])
    half_inverse = np.stack([split_table(table[order].T).T for order in orders])
    blocks = count_pz * PIECES
    units = species * PIECES
    groups = rows_x // blocks
    strip = rows_x * SUBLANES
    f32, bf16 = jnp.float32, jnp.bfloat16
    hbm = pl.BlockSpec(memory_space=pltpu.HBM)
    dma = pltpu.SemaphoreType.DMA

    def far(array):
        return pltpu.with_memory_space_constraint(array, pltpu.HBM)

    return pl.pallas_call(
        kernel,
        out_shape=jax.ShapeDtypeStruct(concentration.shape, f32),
        in_specs=[hbm] * 7,
        out_specs=pl.BlockSpec(memory_space=pltpu.VMEM),
        scratch_shapes=[
            pltpu.SMEM(mobility.shape, f32),
            pltpu.SMEM(kappa.shape, f32),
            pltpu.SMEM(well_depth.shape, f32),
            pltpu.VMEM((species, rows_x, rows_y, n), f32),
            pltpu.VMEM(square_tables.shape, bf16),
            pltpu.VMEM(half_forward.shape[1:], bf16),
            pltpu.VMEM(half_inverse.shape[1:], bf16),
            pltpu.VMEM((2, rows_x, rows_y, n), f32),
            pltpu.VMEM((species, rows_x, rows_y, n), f32),
            pltpu.VMEM((species, n), f32),
            pltpu.VMEM((species, n), f32),
            pltpu.VMEM((2 * units, count_pz, groups, rows_y, n), f32),
            pltpu.VMEM((2 * units, groups, n, n), f32),
            pltpu.VMEM((2 * units, strip, n), f32),
            pltpu.VMEM((2 * units, strip, n), f32),
            pltpu.VMEM((units, 2, strip, n), f32),
            pltpu.VMEM((units, 2, strip, n), f32),
            pltpu.VMEM((units, 2, strip, n), f32),
            pltpu.VMEM((units, strip, n), f32),
            pltpu.VMEM((units, strip, n), f32),
            pltpu.VMEM((units, count_pz, groups, rows_y, n), f32),
            pltpu.VMEM((units, count_pz, groups, rows_y, n), f32),
            dma((groups + 6,)), dma((2,)), dma((groups + 1,)), dma((5,)),
            dma((units + 1,)), dma((SLOTS, SUBLANES // 2)), dma((SLOTS + STEPS,)), dma((SLOTS,)),
            dma((species,)),
        ],
        compiler_params=pltpu.CompilerParams(
            collective_id=0, has_side_effects=True, vmem_limit_bytes=46 * 1024 * 1024
        ),
        name="step",
    )(*(
        far(jnp.asarray(each)) for each in (
            concentration, mobility, kappa, well_depth, square_tables, half_forward, half_inverse
        )
    ))


def per_device(concentration, mobility, kappa, well_depth):
    species, rows_x, rows_y, n = concentration.shape
    count_sp, count_py, count_pz = (lax.axis_size(name) for name in ("sp", "py", "pz"))
    cube = rows_x * count_py == n and rows_y * count_pz == n and n == 128
    blocks = count_pz * PIECES
    whole = n == SUBLANES * blocks and rows_x % (2 * blocks) == 0 and rows_y % SUBLANES == 0
    if cube and whole and count_sp == 2 and count_py == 4 and count_pz == 4 and species == 4:
        return per_device_kernel(concentration, mobility, kappa, well_depth)
    return per_device_general(concentration, mobility, kappa, well_depth)


def solution(mesh):
    in_specs = (P("sp", "py", "pz", None), P(), P(), P("sp"))
    out_specs = P("sp", "py", "pz", None)
    return jax.shard_map(
        per_device, mesh=mesh, in_specs=in_specs, out_specs=out_specs, check_vma=False
    )
```

```python
import functools
import math

import jax
import jax.numpy as jnp
import numpy as np
from jax import lax
from jax.experimental import pallas as pl
from jax.experimental.pallas import tpu as pltpu
from jax.sharding import PartitionSpec as P


def tables(count):
    modes = jnp.arange(count, dtype=jnp.int32)
    product = modes[:, None] * modes[None, :] % count
    angle = 2.0 * math.pi * product.astype(jnp.float32) / count
    return (jnp.cos(angle), jnp.sin(angle))


def wave_square(index, count):
    freq = jnp.where(index < count // 2, index, index - count).astype(jnp.float32)
    return (2.0 * math.pi * freq / count) ** 2


def contract(form, values, table):
    return jnp.einsum(form, values, table, precision=lax.Precision.HIGHEST)


def rotate(spectrum, form, count, forward):
    cosine, sine = tables(count)
    real_part, imag_part = (spectrum[0], spectrum[1])
    real_cos = contract(form, real_part, cosine)
    real_sin = contract(form, real_part, sine)
    imag_cos = contract(form, imag_part, cosine)
    imag_sin = contract(form, imag_part, sine)
    if forward:
        return jnp.stack([real_cos + imag_sin, imag_cos - real_sin])
    return jnp.stack([real_cos - imag_sin, imag_cos + real_sin])


def per_device_general(concentration, mobility, kappa, well_depth):
    local_species, rows_x, rows_y, depth = concentration.shape
    count_sp = lax.axis_size("sp")
    count_py = lax.axis_size("py")
    count_pz = lax.axis_size("pz")
    full_x = rows_x * count_py
    full_y = rows_y * count_pz
    half_depth = depth // 2
    bulk = well_depth[:, None, None, None] * (
        concentration * concentration * concentration - concentration
    )
    fields = jnp.stack([concentration, bulk])
    cosine, sine = tables(depth)
    alternate = (1 - 2 * (jnp.arange(depth, dtype=jnp.int32) % 2)).astype(jnp.float32)
    spectrum = jnp.stack(
        [
            contract("fsxyz,zk->fsxyk", fields, cosine[:, :half_depth]),
            -contract("fsxyz,zk->fsxyk", fields, sine[:, :half_depth]),
        ]
    )
    spectrum = lax.all_to_all(spectrum, "pz", split_axis=5, concat_axis=4, tiled=True)
    own_lines = spectrum.shape[5]
    highest = contract("fsxyz,z->fsxy", fields, alternate)
    highest = lax.all_gather(highest, "pz", axis=3, tiled=True)
    highest = jnp.stack([highest, jnp.zeros_like(highest)])[..., None]
    spectrum = jnp.concatenate([spectrum, highest], axis=5)
    z_modes = jnp.concatenate(
        [
            lax.axis_index("pz") * own_lines + jnp.arange(own_lines, dtype=jnp.int32),
            jnp.full((1,), half_depth, jnp.int32),
        ]
    )
    spectrum = rotate(spectrum, "fsxyz,yk->fsxkz", full_y, True)
    spectrum = lax.all_to_all(
        lax.all_to_all(spectrum, "sp", split_axis=4, concat_axis=2, tiled=True),
        "py",
        split_axis=4,
        concat_axis=3,
        tiled=True,
    )
    spectrum = rotate(spectrum, "fsxyz,xk->fskyz", full_x, True)
    narrow = spectrum.shape[4]
    lines = spectrum.shape[5]
    y_start = (lax.axis_index("sp") * count_py + lax.axis_index("py")) * narrow
    ksq_x = wave_square(jnp.arange(full_x, dtype=jnp.int32), full_x)
    ksq_y = wave_square(y_start + jnp.arange(narrow, dtype=jnp.int32), full_y)
    ksq_z = wave_square(z_modes, depth)
    ksq = ksq_x[:, None, None] + ksq_y[None, :, None] + ksq_z[None, None, :]
    c_hat = spectrum[:, 0]
    drive = spectrum[:, 1] + kappa[None, :, None, None, None] * ksq[None, None] * c_hat
    mix = jnp.einsum("ij,rjxyz->rixyz", mobility, drive, precision=lax.Precision.HIGHEST)
    stiff = 0.5 * (jnp.diagonal(mobility) * kappa)[:, None, None, None] * (ksq * ksq)[None]
    new_hat = (c_hat * (1.0 + stiff)[None] - 0.5 * ksq[None, None] * mix) / (1.0 + stiff)[None]
    new_hat = rotate(new_hat, "sxyz,xk->skyz", full_x, False)
    moved = lax.all_to_all(
        lax.all_to_all(new_hat, "sp", split_axis=1, concat_axis=3, tiled=True),
        "py",
        split_axis=2,
        concat_axis=3,
        tiled=True,
    )
    moved = moved.reshape(2, local_species, rows_x, count_py, count_sp, narrow, lines)
    moved = moved.transpose(0, 1, 2, 4, 3, 5, 6).reshape(2, local_species, rows_x, full_y, lines)
    moved = rotate(moved, "sxyz,yk->sxkz", full_y, False)
    main = moved[..., : lines - 1]
    highest = moved[0, :, :, :, lines - 1]
    main = lax.all_to_all(main, "pz", split_axis=3, concat_axis=4, tiled=True)
    highest = lax.dynamic_slice_in_dim(highest, lax.axis_index("pz") * rows_y, rows_y, 2)
    weight = jnp.where(jnp.arange(half_depth, dtype=jnp.int32) == 0, 1.0, 2.0).astype(jnp.float32)
    result = contract("sxyk,kz->sxyz", main[0] * weight, cosine[:half_depth]) - contract(
        "sxyk,kz->sxyz", main[1] * weight, sine[:half_depth]
    )
    result = result + highest[..., None] * alternate[None, None, None, :]
    return result * (1.0 / (full_x * full_y * depth))


PIECES = 4
SUBLANES = 8
SLOTS = 5
STEPS = 10
LAG = 4
DIRECT = 3
EARLY = 2


def basis(count):
    grid = np.arange(count)
    mode = np.arange(count)
    freq = np.minimum(mode, count - mode)
    angle = 2.0 * np.pi * (grid[:, None] * freq[None, :] % count) / count
    table = np.where(mode[None, :] <= count // 2, np.cos(angle), np.sin(angle))
    single = (mode == 0) | (2 * mode == count)
    return table * np.sqrt(np.where(single, 1.0, 2.0) / count)[None, :]


def split_table(table):
    table = table.astype(np.float32)
    high = table.astype(jnp.bfloat16)
    low = (table - high.astype(np.float32)).astype(jnp.bfloat16)
    row = np.concatenate([high, low], axis=1)
    return np.concatenate([row, row], axis=0)


def split(values, axis):
    high = values.astype(jnp.bfloat16)
    low = (values - high.astype(jnp.float32)).astype(jnp.bfloat16)
    return jnp.concatenate([high, low], axis=axis)


def from_right(values, table):
    count = values.shape[1]
    out = jnp.dot(split(values, 1), table, preferred_element_type=jnp.float32)
    return out[:, :count] + out[:, count:]


def from_left(table, values):
    count = table.shape[0] // 2
    out = jnp.dot(table, split(values, 0), preferred_element_type=jnp.float32)
    return out[:count] + out[count:]


def swap_blocks(parts, width):
    parts = list(parts)
    axis = parts[0].ndim - 1
    lanes = parts[0].shape[axis]
    block = lax.broadcasted_iota(jnp.int32, parts[0].shape, axis) // width
    half = len(parts) // 2
    while half:
        low_side = (block // half) % 2 == 0
        for first in range(len(parts)):
            if (first // half) % 2 == 0:
                one, two = parts[first], parts[first + half]
                parts[first] = jnp.where(low_side, one, pltpu.roll(two, half * width, axis))
                parts[first + half] = jnp.where(
                    low_side, pltpu.roll(one, lanes - half * width, axis), two
                )
        half //= 2
    return parts


def kernel(
    conc_hbm, mobility_hbm, kappa_hbm, well_depth_hbm, square_hbm, half_f_hbm, half_i_hbm, out,
    mobility, kappa, well_depth, conc, square_tables, half_f, half_i, own_mix,
    other, depths, other_depths, z_out, z_in, y_out, y_in, near, x_out, x_in, b_out, b_in, w_out, w_in,
    load, pair_sent, pair_got, sent, zr, yr, xr, br, wr,
):
    species, rows_x, rows_y, n = conc.shape
    me_sp, me_py, me_pz = lax.axis_index("sp"), lax.axis_index("py"), lax.axis_index("pz")
    count_pz = n // rows_y
    blocks = count_pz * PIECES
    units = species * PIECES
    last = units - 1
    width = n // blocks
    groups = rows_x // blocks
    sub = SUBLANES
    quarters = sub // 2
    mesh_id = pl.DeviceIdType.MESH

    half = me_py // 2
    inner = lax.rem(me_py + half, 2) == 1
    outer = jnp.logical_not(inner)
    buddy = {"sp": me_sp, "py": me_py + 1 - 2 * lax.rem(me_py, 2), "pz": me_pz}
    across_py = 3 - me_py
    far_py = lax.rem(me_py + 2, 4)
    across = {"sp": me_sp, "py": across_py, "pz": me_pz}
    partner = {"sp": 1 - me_sp, "py": me_py, "pz": me_pz}
    others_pz = [3 - me_pz, me_pz + 1 - 2 * lax.rem(me_pz, 2), lax.rem(me_pz + 2, 4)]

    def along_pz(peer):
        return {"sp": me_sp, "py": me_py, "pz": peer}

    barrier = pltpu.get_barrier_semaphore()
    peers = [partner, buddy] + [along_pz(peer) for peer in others_pz]
    for peer in peers:
        pl.semaphore_signal(barrier, inc=1, device_id=peer, device_id_type=mesh_id)

    @pl.when(inner)
    def _():
        pl.semaphore_signal(barrier, inc=1, device_id=across, device_id_type=mesh_id)

    lots = 2 * groups
    lot_rows = rows_x // lots

    def lot(i):
        return pl.ds(i * lot_rows, lot_rows)

    def group(g):
        return pl.ds(g * blocks, blocks)

    moves = [(conc_hbm.at[:, group(g)], conc.at[:, group(g)]) for g in range(groups)]
    moves += [
        (well_depth_hbm, well_depth), (mobility_hbm, mobility), (kappa_hbm, kappa),
        (square_hbm, square_tables), (half_f_hbm.at[half], half_f), (half_i_hbm.at[half], half_i),
    ]
    loads = [
        pltpu.make_async_copy(source, target, load.at[i])
        for i, (source, target) in enumerate(moves)
    ]
    for copy in loads:
        copy.start()
    conc_loads, small_loads, table_loads = loads[:groups], loads[groups:-3], loads[-3:]
    right_f, left_f, left_i, right_i = (square_tables.at[i] for i in range(4))
    for copy in small_loads:
        copy.wait()
    for t in range(species):
        depths[t : t + 1, :] = jnp.full((1, n), well_depth[t], jnp.float32)
    pl.semaphore_wait(barrier, len(peers) + jnp.where(inner, 1, 0))

    def remote(source, target, send, recv, peer):
        return pltpu.make_async_remote_copy(
            src_ref=source, dst_ref=target, send_sem=send, recv_sem=recv,
            device_id=peer, device_id_type=mesh_id,
        )

    def waiter(lines, sem):
        return pltpu.make_async_remote_copy(
            src_ref=lines, dst_ref=lines, send_sem=sem, recv_sem=sem,
            device_id=partner, device_id_type=mesh_id,
        )

    depth_pair = remote(depths, other_depths, pair_sent.at[1], pair_got.at[lots], partner)
    pair = [
        remote(
            conc.at[:, lot(i)], other.at[:, lot(i)], pair_sent.at[0], pair_got.at[i], partner
        )
        for i in range(lots)
    ]
    for g in range(groups):
        conc_loads[g].wait()
        pair[2 * g].start()
        if g == 0:
            depth_pair.start()
        pair[2 * g + 1].start()

    y_rows = pl.ds(pl.multiple_of(me_pz * rows_y, rows_y), rows_y)
    z_sent, y_sent, x_sent, b_sent, w_sent = (sent.at[i] for i in range(5))

    def z_copy(chunk, peer, part):
        slot = chunk if chunk < 2 else chunk // 2 + 1
        if chunk >= 4 * PIECES:
            slot = 2 * PIECES - 1 + chunk // (2 * PIECES)
        return remote(
            z_out.at[chunk, peer, part], z_in.at[chunk, part, y_rows], z_sent,
            zr.at[slot], along_pz(peer),
        )

    def z_all(first, count, slot):
        lines = z_in.at[pl.ds(first, count), :, pl.ds(0, (count_pz - 1) * rows_y)]
        return waiter(lines, zr.at[slot])

    def rows_of(q):
        return pl.ds(pl.multiple_of(2 * rows_x * q, 2 * rows_x), 2 * rows_x)

    def slot_of(one):
        return lax.rem(one, SLOTS)

    def x_slot(one):
        return lax.rem(one, SLOTS + 1)

    def y_copy(one, f, q):
        chunk, rows = 2 * one + f, rows_of(q)
        return remote(
            y_out.at[chunk, rows], y_in.at[chunk, rows], y_sent, yr.at[slot_of(one), q], buddy
        )

    def y_all(one, q):
        return waiter(y_in.at[pl.ds(2 * one, 2), rows_of(q)], yr.at[slot_of(one), q])

    def x_copy(one, part, q):
        rows = rows_of(q)
        got = x_slot(one)
        target = across
        if part:
            got = SLOTS + 1 + lax.rem(one * quarters + q, STEPS)
            direct = (one * quarters + q) // (units * quarters - DIRECT)
            target = {"sp": me_sp, "py": across_py + direct * (far_py - across_py), "pz": me_pz}
        return remote(
            x_out.at[one, part, rows], x_in.at[one, part, rows], x_sent, xr.at[got], target
        )

    def x_all(one):
        return waiter(x_in.at[one, 0], xr.at[x_slot(one)])

    def b_all(one):
        return waiter(b_in.at[one], br.at[slot_of(one)])

    def w_copy(one, peer, part, slot):
        return remote(
            w_out.at[one, peer, part], w_in.at[one, me_pz, part], w_sent, wr.at[slot],
            along_pz(peer),
        )

    def w_all(one, count):
        lines = w_in.at[pl.ds(PIECES * one, count), pl.ds(0, count_pz - 1)]
        return waiter(lines, wr.at[one])

    def w_last(g):
        lines = w_in.at[last, pl.ds(0, count_pz - 1), pl.ds(g, 1)]
        return waiter(lines, wr.at[species + g])

    def terms_of(one, side, field, depth):
        own_i = me_sp * species + one
        terms = []
        for t in range(species):
            j = side * species + t
            weight = mobility[own_i, j]
            terms.append((field, t, weight * depth[t : t + 1, :], weight * kappa[j]))
        return terms

    def mixed(terms, x, first=None, second=None):
        for field, t, bulk_weight, conc_weight in terms:
            c = field[t, x]
            a = bulk_weight * (c * c * c - c)
            b = conc_weight * c
            first = a if first is None else first + a
            second = b if second is None else second + b
        return first, second

    def z_part(one, g, opening=False):
        own = terms_of(one, me_sp, conc, depths)
        if opening and g == 0:
            for x in range(rows_x):
                own_mix[0, x], own_mix[1, x] = mixed(own, x)
            depth_pair.wait_recv()
        others = terms_of(one, 1 - me_sp, other, other_depths)
        parts = 2 if opening else 1
        modes = [[], []]
        for i in range(parts):
            if opening:
                pair[2 * g + i].wait_recv()
            bulk_mix, conc_mix = [], []
            for block in range(i * blocks // parts, (i + 1) * blocks // parts):
                x = g * blocks + block
                if opening:
                    first, second = mixed(others, x, own_mix[0, x], own_mix[1, x])
                else:
                    first, second = mixed(own + others, x)
                bulk_mix.append(first)
                conc_mix.append(second)
            lines = from_right(jnp.concatenate(bulk_mix + conc_mix, axis=0), right_f[...])
            lines = lines.reshape(2, blocks // parts, rows_y, n)
            for f in range(2):
                modes[f] += [lines[f, block] for block in range(blocks // parts)]
        for f in range(2):
            swapped = swap_blocks(modes[f], width)
            for block in range(blocks):
                unit = PIECES * one + block % PIECES
                z_out[2 * unit + f, block // PIECES, g] = swapped[block]
            if opening:
                for peer in others_pz:
                    z_copy(f, peer, pl.ds(g, 1)).start()
        if g == groups - 1:
            for c in range(2 if opening else 0, 2 * PIECES):
                for peer in others_pz:
                    z_copy(2 * PIECES * one + c, peer, pl.ds(0, groups)).start()
            for c in range(2 * PIECES):
                chunk = 2 * PIECES * one + c
                z_in[chunk, :, y_rows] = z_out[chunk, me_pz]

    def y_chunk(chunk):
        for g in range(0, groups, 2):
            lines = jnp.concatenate([z_in[chunk, g], z_in[chunk, g + 1]], axis=1)
            modes = from_left(left_f[...], lines)
            for h in range(2):
                part = modes[:, h * n : (h + 1) * n].reshape(blocks, sub, n)
                swapped = swap_blocks([part[b] for b in range(blocks)], width)
                for block in range(blocks):
                    x = (g + h) * blocks + block
                    y_out[chunk, pl.ds(x, sub, stride=rows_x), :] = swapped[block]

    def y_send(one):
        @pl.when(outer)
        def _():
            for q in range(quarters):
                for f in range(2):
                    y_copy(one, f, q).start()

    def square(index):
        freq = jnp.minimum(index, n - index).astype(jnp.float32)
        root = freq * (2.0 * math.pi / n)
        return root * root

    lane = lax.broadcasted_iota(jnp.int32, (1, n), 1)
    ksq_x = square(lax.broadcasted_iota(jnp.int32, (n, 1), 0))

    def x_quarter(one, q):
        y_all(one, q).wait_recv()
        own_i = me_sp * species + one // PIECES
        piece = me_pz * PIECES + lax.rem(one, PIECES)
        ksq_z = square(piece * width + lane % width)
        half_stiff = 0.5 * (mobility[own_i, own_i] * kappa[own_i])

        def line_rows(h):
            return pl.ds(pl.multiple_of((2 * q + h) * rows_x, rows_x), rows_x)

        both, ksq = [], []
        for f in range(2):
            chunk = 2 * one + f
            both.append(from_left(half_f[...], jnp.concatenate([
                jnp.concatenate([
                    field[chunk, line_rows(h), :] for field in (y_out, y_in)
                ], axis=0)
                for h in range(2)
            ], axis=1)))
        for h in range(2):
            ksq_y = square((lane // width) * sub + (2 * q + h))
            ksq.append(ksq_x + (ksq_y + ksq_z))
        ksq = jnp.concatenate(ksq, axis=1)
        drop = 0.5 * ksq * (both[0] + ksq * both[1]) / (1.0 + half_stiff * (ksq * ksq))
        lines = from_left(half_i[...], drop)
        for h in range(2):
            for i, (field, part) in enumerate([(near, 0), (near, 1), (x_out, 0), (x_out, 1)]):
                field[one, part, line_rows(h), :] = lines[
                    i * rows_x : (i + 1) * rows_x, h * n : (h + 1) * n
                ]
        x_copy(one, 1, q).start()
        x_copy(one, 0, q).start()

        @pl.when(one * quarters + q >= units * quarters - DIRECT)
        def _():
            rows = rows_of(q)
            remote(
                near.at[last, 1, rows], b_in.at[last, rows], b_sent, br.at[last % SLOTS], buddy
            ).start()

    def combine_quarter(step):
        one, q = step // quarters, lax.rem(step, quarters)
        rows = rows_of(q)
        x_copy(one, 1, q).wait_recv()
        b_out[one, rows, :] = near[one, 1, rows, :] + x_in[one, 1, rows, :]
        remote(
            b_out.at[one, rows], b_in.at[one, rows], b_sent, br.at[slot_of(one)], buddy
        ).start()

    def combine_inner(one):
        x_all(one).wait_recv()
        b_in[one] = near[one, 0] + x_in[one, 0]

    def y_back(one, closing=False):
        for g in range(0, groups, 2):
            pairs = []
            for h in range(2):
                parts = []
                for block in range(blocks):
                    x = (g + h) * blocks + block
                    parts.append(b_in[one, pl.ds(x, sub, stride=rows_x), :])
                swapped = swap_blocks(parts, width)
                pairs.append(jnp.stack(swapped, axis=0).reshape(n, n))
            lines = from_left(left_i[...], jnp.concatenate(pairs, axis=1))
            for h in range(2):
                part = lines[:, h * n : (h + 1) * n].reshape(count_pz, rows_y, n)
                w_out[one, :, g + h] = part
        if closing:
            for g in range(groups):
                for peer in others_pz:
                    w_copy(one, peer, pl.ds(g, 1), species + g).start()
        else:
            for peer in others_pz:
                w_copy(one, peer, pl.ds(0, groups), one // PIECES).start()
        w_in[one, me_pz] = w_out[one, me_pz]

    def back(one):
        @pl.when(inner)
        def _():
            combine_inner(one)

        @pl.when(outer)
        def _():
            b_all(one).wait_recv()

        y_back(one)

    def z_back(one, closing=False):
        w_all(one, PIECES - 1 if closing else PIECES).wait_recv()
        for g in range(groups):
            if closing:
                w_last(g).wait_recv()
            rows = swap_blocks([
                w_in[PIECES * one + block % PIECES, block // PIECES, g]
                for block in range(blocks)
            ], width)
            lines = from_right(jnp.concatenate(rows, axis=0), right_i[...])
            lines = lines.reshape(blocks, rows_y, n)
            for block in range(blocks):
                x = g * blocks + block
                out[one, x] = conc[one, x] - lines[block]

    table_loads[0].wait()
    for g in range(groups):
        z_part(0, g, True)
    for copy in table_loads[1:]:
        copy.wait()
    for g in range(groups):
        z_part(1, g)
    for f in range(2):
        z_all(f, 1, f).wait_recv()
        y_chunk(f)

        @pl.when(outer)
        def _(f=f):
            for q in range(EARLY):
                y_copy(0, f, q).start()

    @pl.when(outer)
    def _():
        for q in range(EARLY, quarters):
            for f in range(2):
                y_copy(0, f, q).start()

    z_all(2, 2, 2).wait_recv()
    for f in range(2):
        y_chunk(2 + f)
    y_send(1)
    extra = {}
    for one in range(2, species):
        for g in range(groups):
            extra[2 + (one - 2) * groups + g] = functools.partial(z_part, one, g)
    for one in range(species - 1):
        extra[units + 1 - 2 * (species - 1 - one)] = functools.partial(z_back, one)

    def middle(step, _):
        one, q = step // quarters, lax.rem(step, quarters)
        ahead, behind = one + 2, one - 2

        @pl.when(jnp.logical_and(inner, step >= LAG))
        def _():
            combine_quarter(step - LAG)

        @pl.when(inner)
        def _():
            x_quarter(one, q)

        for unit, work in extra.items():
            @pl.when(jnp.logical_and(one == unit, q == 0))
            def _(work=work):
                work()

        @pl.when(jnp.logical_and(ahead < 2 * PIECES, q == 1))
        def _():
            z_all(2 * ahead, 2, ahead + 1).wait_recv()

        for each in range(2, species):
            @pl.when(jnp.logical_and(ahead == PIECES * each, q == 1))
            def _(each=each):
                z_all(2 * PIECES * each, 2 * PIECES, 2 * PIECES - 1 + each).wait_recv()

        @pl.when(jnp.logical_and(ahead < units, jnp.logical_and(q > 0, q < 3)))
        def _():
            y_chunk(2 * ahead + q - 1)

        @pl.when(jnp.logical_and(ahead < units, q == 2))
        def _():
            y_send(ahead)

        @pl.when(jnp.logical_and(behind >= 0, q == 3))
        def _():
            back(behind)

        return 0

    steps = units * quarters
    lax.fori_loop(0, steps, middle, 0)

    def returns(step, _):
        combine_quarter(step)
        return 0

    @pl.when(inner)
    def _():
        lax.fori_loop(steps - LAG, steps - quarters, returns, 0)

    back(last - 1)

    @pl.when(inner)
    def _():
        lax.fori_loop(steps - quarters, steps - DIRECT, returns, 0)
        combine_inner(last)

    @pl.when(outer)
    def _():
        b_all(last).wait_recv()
        for q in range(quarters - DIRECT, quarters):
            x_copy(last, 1, q).wait_recv()
            rows = rows_of(q)
            b_in[last, rows, :] = b_in[last, rows, :] + x_in[last, 1, rows, :]

    y_back(last, True)
    z_back(species - 1, True)

    depth_pair.wait_send()
    waiter(conc, pair_sent.at[0]).wait_send()
    waiter(z_out.at[:, pl.ds(0, count_pz - 1)], z_sent).wait_send()

    @pl.when(outer)
    def _():
        waiter(y_out, y_sent).wait_send()

    @pl.when(inner)
    def _():
        waiter(x_out, x_sent).wait_send()
        waiter(b_out, b_sent).wait_send()

    waiter(w_out.at[:, pl.ds(0, count_pz - 1)], w_sent).wait_send()


def per_device_kernel(concentration, mobility, kappa, well_depth):
    species, rows_x, rows_y, n = concentration.shape
    count_py, count_pz = lax.axis_size("py"), lax.axis_size("pz")
    table = basis(n)
    forward = split_table(table)
    inverse = split_table(table.T)
    square_tables = np.stack([forward, forward.T, inverse.T, inverse])
    blocks = np.arange(n).reshape(count_py, rows_x)
    orders = [blocks[[1, 0, 2, 3]].reshape(n), blocks[[2, 3, 1, 0]].reshape(n)]
    half_forward = np.stack([split_table(table[order[: n // 2]]).T for order in orders])
    half_inverse = np.stack([split_table(table[order].T).T for order in orders])
    blocks = count_pz * PIECES
    units = species * PIECES
    groups = rows_x // blocks
    strip = rows_x * SUBLANES
    f32, bf16 = jnp.float32, jnp.bfloat16
    hbm = pl.BlockSpec(memory_space=pltpu.HBM)
    dma = pltpu.SemaphoreType.DMA

    def far(array):
        return pltpu.with_memory_space_constraint(array, pltpu.HBM)

    return pl.pallas_call(
        kernel,
        out_shape=jax.ShapeDtypeStruct(concentration.shape, f32),
        in_specs=[hbm] * 7,
        out_specs=pl.BlockSpec(memory_space=pltpu.VMEM),
        scratch_shapes=[
            pltpu.SMEM(mobility.shape, f32),
            pltpu.SMEM(kappa.shape, f32),
            pltpu.SMEM(well_depth.shape, f32),
            pltpu.VMEM((species, rows_x, rows_y, n), f32),
            pltpu.VMEM(square_tables.shape, bf16),
            pltpu.VMEM(half_forward.shape[1:], bf16),
            pltpu.VMEM(half_inverse.shape[1:], bf16),
            pltpu.VMEM((2, rows_x, rows_y, n), f32),
            pltpu.VMEM((species, rows_x, rows_y, n), f32),
            pltpu.VMEM((species, n), f32),
            pltpu.VMEM((species, n), f32),
            pltpu.VMEM((2 * units, count_pz, groups, rows_y, n), f32),
            pltpu.VMEM((2 * units, groups, n, n), f32),
            pltpu.VMEM((2 * units, strip, n), f32),
            pltpu.VMEM((2 * units, strip, n), f32),
            pltpu.VMEM((units, 2, strip, n), f32),
            pltpu.VMEM((units, 2, strip, n), f32),
            pltpu.VMEM((units, 2, strip, n), f32),
            pltpu.VMEM((units, strip, n), f32),
            pltpu.VMEM((units, strip, n), f32),
            pltpu.VMEM((units, count_pz, groups, rows_y, n), f32),
            pltpu.VMEM((units, count_pz, groups, rows_y, n), f32),
            dma((groups + 6,)), dma((2,)), dma((2 * groups + 1,)), dma((5,)),
            dma((2 * PIECES + species - 1,)), dma((SLOTS, SUBLANES // 2)), dma((SLOTS + 1 + STEPS,)), dma((SLOTS,)),
            dma((species + groups,)),
        ],
        compiler_params=pltpu.CompilerParams(
            collective_id=0, has_side_effects=True, vmem_limit_bytes=46 * 1024 * 1024
        ),
        name="step",
    )(*(
        far(jnp.asarray(each)) for each in (
            concentration, mobility, kappa, well_depth, square_tables, half_forward, half_inverse
        )
    ))


def per_device(concentration, mobility, kappa, well_depth):
    species, rows_x, rows_y, n = concentration.shape
    count_sp, count_py, count_pz = (lax.axis_size(name) for name in ("sp", "py", "pz"))
    cube = rows_x * count_py == n and rows_y * count_pz == n and n == 128
    blocks = count_pz * PIECES
    whole = n == SUBLANES * blocks and rows_x % (2 * blocks) == 0 and rows_y % SUBLANES == 0
    if cube and whole and count_sp == 2 and count_py == 4 and count_pz == 4 and species == 4:
        return per_device_kernel(concentration, mobility, kappa, well_depth)
    return per_device_general(concentration, mobility, kappa, well_depth)


def solution(mesh):
    in_specs = (P("sp", "py", "pz", None), P(), P(), P("sp"))
    out_specs = P("sp", "py", "pz", None)
    return jax.shard_map(
        per_device, mesh=mesh, in_specs=in_specs, out_specs=out_specs, check_vma=False
    )
```

```python
import functools
import math

import jax
import jax.numpy as jnp
import numpy as np
from jax import lax
from jax.experimental import pallas as pl
from jax.experimental.pallas import tpu as pltpu
from jax.sharding import PartitionSpec as P


def tables(count):
    modes = jnp.arange(count, dtype=jnp.int32)
    product = modes[:, None] * modes[None, :] % count
    angle = 2.0 * math.pi * product.astype(jnp.float32) / count
    return (jnp.cos(angle), jnp.sin(angle))


def wave_square(index, count):
    freq = jnp.where(index < count // 2, index, index - count).astype(jnp.float32)
    return (2.0 * math.pi * freq / count) ** 2


def contract(form, values, table):
    return jnp.einsum(form, values, table, precision=lax.Precision.HIGHEST)


def rotate(spectrum, form, count, forward):
    cosine, sine = tables(count)
    real_part, imag_part = (spectrum[0], spectrum[1])
    real_cos = contract(form, real_part, cosine)
    real_sin = contract(form, real_part, sine)
    imag_cos = contract(form, imag_part, cosine)
    imag_sin = contract(form, imag_part, sine)
    if forward:
        return jnp.stack([real_cos + imag_sin, imag_cos - real_sin])
    return jnp.stack([real_cos - imag_sin, imag_cos + real_sin])


def per_device_general(concentration, mobility, kappa, well_depth):
    local_species, rows_x, rows_y, depth = concentration.shape
    count_sp = lax.axis_size("sp")
    count_py = lax.axis_size("py")
    count_pz = lax.axis_size("pz")
    full_x = rows_x * count_py
    full_y = rows_y * count_pz
    half_depth = depth // 2
    bulk = well_depth[:, None, None, None] * (
        concentration * concentration * concentration - concentration
    )
    fields = jnp.stack([concentration, bulk])
    cosine, sine = tables(depth)
    alternate = (1 - 2 * (jnp.arange(depth, dtype=jnp.int32) % 2)).astype(jnp.float32)
    spectrum = jnp.stack(
        [
            contract("fsxyz,zk->fsxyk", fields, cosine[:, :half_depth]),
            -contract("fsxyz,zk->fsxyk", fields, sine[:, :half_depth]),
        ]
    )
    spectrum = lax.all_to_all(spectrum, "pz", split_axis=5, concat_axis=4, tiled=True)
    own_lines = spectrum.shape[5]
    highest = contract("fsxyz,z->fsxy", fields, alternate)
    highest = lax.all_gather(highest, "pz", axis=3, tiled=True)
    highest = jnp.stack([highest, jnp.zeros_like(highest)])[..., None]
    spectrum = jnp.concatenate([spectrum, highest], axis=5)
    z_modes = jnp.concatenate(
        [
            lax.axis_index("pz") * own_lines + jnp.arange(own_lines, dtype=jnp.int32),
            jnp.full((1,), half_depth, jnp.int32),
        ]
    )
    spectrum = rotate(spectrum, "fsxyz,yk->fsxkz", full_y, True)
    spectrum = lax.all_to_all(
        lax.all_to_all(spectrum, "sp", split_axis=4, concat_axis=2, tiled=True),
        "py",
        split_axis=4,
        concat_axis=3,
        tiled=True,
    )
    spectrum = rotate(spectrum, "fsxyz,xk->fskyz", full_x, True)
    narrow = spectrum.shape[4]
    lines = spectrum.shape[5]
    y_start = (lax.axis_index("sp") * count_py + lax.axis_index("py")) * narrow
    ksq_x = wave_square(jnp.arange(full_x, dtype=jnp.int32), full_x)
    ksq_y = wave_square(y_start + jnp.arange(narrow, dtype=jnp.int32), full_y)
    ksq_z = wave_square(z_modes, depth)
    ksq = ksq_x[:, None, None] + ksq_y[None, :, None] + ksq_z[None, None, :]
    c_hat = spectrum[:, 0]
    drive = spectrum[:, 1] + kappa[None, :, None, None, None] * ksq[None, None] * c_hat
    mix = jnp.einsum("ij,rjxyz->rixyz", mobility, drive, precision=lax.Precision.HIGHEST)
    stiff = 0.5 * (jnp.diagonal(mobility) * kappa)[:, None, None, None] * (ksq * ksq)[None]
    new_hat = (c_hat * (1.0 + stiff)[None] - 0.5 * ksq[None, None] * mix) / (1.0 + stiff)[None]
    new_hat = rotate(new_hat, "sxyz,xk->skyz", full_x, False)
    moved = lax.all_to_all(
        lax.all_to_all(new_hat, "sp", split_axis=1, concat_axis=3, tiled=True),
        "py",
        split_axis=2,
        concat_axis=3,
        tiled=True,
    )
    moved = moved.reshape(2, local_species, rows_x, count_py, count_sp, narrow, lines)
    moved = moved.transpose(0, 1, 2, 4, 3, 5, 6).reshape(2, local_species, rows_x, full_y, lines)
    moved = rotate(moved, "sxyz,yk->sxkz", full_y, False)
    main = moved[..., : lines - 1]
    highest = moved[0, :, :, :, lines - 1]
    main = lax.all_to_all(main, "pz", split_axis=3, concat_axis=4, tiled=True)
    highest = lax.dynamic_slice_in_dim(highest, lax.axis_index("pz") * rows_y, rows_y, 2)
    weight = jnp.where(jnp.arange(half_depth, dtype=jnp.int32) == 0, 1.0, 2.0).astype(jnp.float32)
    result = contract("sxyk,kz->sxyz", main[0] * weight, cosine[:half_depth]) - contract(
        "sxyk,kz->sxyz", main[1] * weight, sine[:half_depth]
    )
    result = result + highest[..., None] * alternate[None, None, None, :]
    return result * (1.0 / (full_x * full_y * depth))


PIECES = 4
SUBLANES = 8
SLOTS = 5
STEPS = 8
LAG = 4
DIRECT = 3
EARLY = 2


def basis(count):
    grid = np.arange(count)
    mode = np.arange(count)
    freq = np.minimum(mode, count - mode)
    angle = 2.0 * np.pi * (grid[:, None] * freq[None, :] % count) / count
    table = np.where(mode[None, :] <= count // 2, np.cos(angle), np.sin(angle))
    single = (mode == 0) | (2 * mode == count)
    return table * np.sqrt(np.where(single, 1.0, 2.0) / count)[None, :]


def split_table(table):
    table = table.astype(np.float32)
    high = table.astype(jnp.bfloat16)
    low = (table - high.astype(np.float32)).astype(jnp.bfloat16)
    row = np.concatenate([high, low], axis=1)
    return np.concatenate([row, row], axis=0)


def split(values, axis):
    high = values.astype(jnp.bfloat16)
    low = (values - high.astype(jnp.float32)).astype(jnp.bfloat16)
    return jnp.concatenate([high, low], axis=axis)


def from_right(values, table):
    count = values.shape[1]
    out = jnp.dot(split(values, 1), table, preferred_element_type=jnp.float32)
    return out[:, :count] + out[:, count:]


def from_left(table, values):
    count = table.shape[0] // 2
    out = jnp.dot(table, split(values, 0), preferred_element_type=jnp.float32)
    return out[:count] + out[count:]


def swap_blocks(parts, width):
    parts = list(parts)
    axis = parts[0].ndim - 1
    lanes = parts[0].shape[axis]
    block = lax.broadcasted_iota(jnp.int32, parts[0].shape, axis) // width
    half = len(parts) // 2
    while half:
        low_side = (block // half) % 2 == 0
        for first in range(len(parts)):
            if (first // half) % 2 == 0:
                one, two = parts[first], parts[first + half]
                parts[first] = jnp.where(low_side, one, pltpu.roll(two, half * width, axis))
                parts[first + half] = jnp.where(
                    low_side, pltpu.roll(one, lanes - half * width, axis), two
                )
        half //= 2
    return parts


def kernel(
    conc_hbm, mobility_hbm, kappa_hbm, well_depth_hbm, square_hbm, half_f_hbm, half_i_hbm, out,
    mobility, kappa, well_depth, conc, square_tables, half_f, half_i, own_mix,
    other, depths, other_depths, z_out, z_in, y_out, y_in, near, x_out, x_in, b_out, b_in, w_out, w_in,
    load, pair_sent, pair_got, sent, zr, yr, xr, br, wr,
):
    species, rows_x, rows_y, n = conc.shape
    me_sp, me_py, me_pz = lax.axis_index("sp"), lax.axis_index("py"), lax.axis_index("pz")
    count_pz = n // rows_y
    blocks = count_pz * PIECES
    units = species * PIECES
    last = units - 1
    width = n // blocks
    groups = rows_x // blocks
    sub = SUBLANES
    quarters = sub // 2
    mesh_id = pl.DeviceIdType.MESH

    half = me_py // 2
    inner = lax.rem(me_py + half, 2) == 1
    outer = jnp.logical_not(inner)
    buddy = {"sp": me_sp, "py": me_py + 1 - 2 * lax.rem(me_py, 2), "pz": me_pz}
    across_py = 3 - me_py
    far_py = lax.rem(me_py + 2, 4)
    across = {"sp": me_sp, "py": across_py, "pz": me_pz}
    partner = {"sp": 1 - me_sp, "py": me_py, "pz": me_pz}
    others_pz = [3 - me_pz, me_pz + 1 - 2 * lax.rem(me_pz, 2), lax.rem(me_pz + 2, 4)]

    def along_pz(peer):
        return {"sp": me_sp, "py": me_py, "pz": peer}

    barrier = pltpu.get_barrier_semaphore()
    peers = [partner, buddy] + [along_pz(peer) for peer in others_pz]
    for peer in peers:
        pl.semaphore_signal(barrier, inc=1, device_id=peer, device_id_type=mesh_id)

    @pl.when(inner)
    def _():
        pl.semaphore_signal(barrier, inc=1, device_id=across, device_id_type=mesh_id)

    lots = 2 * groups
    lot_rows = rows_x // lots

    def lot(i):
        return pl.ds(i * lot_rows, lot_rows)

    def group(g):
        return pl.ds(g * blocks, blocks)

    moves = [(conc_hbm.at[:, group(g)], conc.at[:, group(g)]) for g in range(groups)]
    moves += [
        (well_depth_hbm, well_depth), (mobility_hbm, mobility), (kappa_hbm, kappa),
        (square_hbm, square_tables), (half_f_hbm.at[half], half_f), (half_i_hbm.at[half], half_i),
    ]
    loads = [
        pltpu.make_async_copy(source, target, load.at[i])
        for i, (source, target) in enumerate(moves)
    ]
    for copy in loads:
        copy.start()
    conc_loads, small_loads, table_loads = loads[:groups], loads[groups:-3], loads[-3:]
    right_f, left_f, left_i, right_i = (square_tables.at[i] for i in range(4))
    for copy in small_loads:
        copy.wait()
    for t in range(species):
        depths[t : t + 1, :] = jnp.full((1, n), well_depth[t], jnp.float32)
    pl.semaphore_wait(barrier, len(peers) + jnp.where(inner, 1, 0))

    def remote(source, target, send, recv, peer):
        return pltpu.make_async_remote_copy(
            src_ref=source, dst_ref=target, send_sem=send, recv_sem=recv,
            device_id=peer, device_id_type=mesh_id,
        )

    def waiter(lines, sem):
        return pltpu.make_async_remote_copy(
            src_ref=lines, dst_ref=lines, send_sem=sem, recv_sem=sem,
            device_id=partner, device_id_type=mesh_id,
        )

    depth_pair = remote(depths, other_depths, pair_sent.at[1], pair_got.at[lots], partner)
    pair = [
        remote(
            conc.at[:, lot(i)], other.at[:, lot(i)], pair_sent.at[0], pair_got.at[i], partner
        )
        for i in range(lots)
    ]
    for g in range(groups):
        conc_loads[g].wait()
        pair[2 * g].start()
        if g == 0:
            depth_pair.start()
        pair[2 * g + 1].start()

    y_rows = pl.ds(pl.multiple_of(me_pz * rows_y, rows_y), rows_y)
    z_sent, y_sent, x_sent, b_sent, w_sent = (sent.at[i] for i in range(5))

    def z_copy(chunk, peer, part):
        slot = chunk if chunk < 2 else chunk // 2 + 1
        if chunk >= 4 * PIECES:
            slot = 2 * PIECES - 1 + chunk // (2 * PIECES)
        return remote(
            z_out.at[chunk, peer, part], z_in.at[chunk, part, y_rows], z_sent,
            zr.at[slot], along_pz(peer),
        )

    def z_all(first, count, slot):
        lines = z_in.at[pl.ds(first, count), :, pl.ds(0, (count_pz - 1) * rows_y)]
        return waiter(lines, zr.at[slot])

    def rows_of(q):
        return pl.ds(pl.multiple_of(2 * rows_x * q, 2 * rows_x), 2 * rows_x)

    def slot_of(one):
        return lax.rem(one, SLOTS)

    def x_slot(one):
        return lax.rem(one, SLOTS + 1)

    def y_copy(one, f, q):
        chunk, rows = 2 * one + f, rows_of(q)
        return remote(
            y_out.at[chunk, rows], y_in.at[chunk, rows], y_sent, yr.at[slot_of(one), q], buddy
        )

    def y_all(one, q):
        return waiter(y_in.at[pl.ds(2 * one, 2), rows_of(q)], yr.at[slot_of(one), q])

    def x_copy(one, part, q):
        rows = rows_of(q)
        got = x_slot(one)
        target = across
        if part:
            got = SLOTS + 1 + lax.rem(one * quarters + q, STEPS)
            direct = (one * quarters + q) // (units * quarters - DIRECT)
            target = {"sp": me_sp, "py": across_py + direct * (far_py - across_py), "pz": me_pz}
        return remote(
            x_out.at[one, part, rows], x_in.at[one, part, rows], x_sent, xr.at[got], target
        )

    def x_all(one):
        return waiter(x_in.at[one, 0], xr.at[x_slot(one)])

    def b_all(one):
        return waiter(b_in.at[one], br.at[slot_of(one)])

    def w_copy(one, peer, part, slot):
        return remote(
            w_out.at[one, peer, part], w_in.at[one, me_pz, part], w_sent, wr.at[slot],
            along_pz(peer),
        )

    def w_all(one, count):
        lines = w_in.at[pl.ds(PIECES * one, count), pl.ds(0, count_pz - 1)]
        return waiter(lines, wr.at[one])

    def w_last(g):
        lines = w_in.at[last, pl.ds(0, count_pz - 1), pl.ds(g, 1)]
        return waiter(lines, wr.at[species + g])

    def terms_of(one, side, field, depth):
        own_i = me_sp * species + one
        terms = []
        for t in range(species):
            j = side * species + t
            weight = mobility[own_i, j]
            terms.append((field, t, weight * depth[t : t + 1, :], weight * kappa[j]))
        return terms

    def mixed(terms, x, first=None, second=None):
        for field, t, bulk_weight, conc_weight in terms:
            c = field[t, x]
            a = bulk_weight * (c * c * c - c)
            b = conc_weight * c
            first = a if first is None else first + a
            second = b if second is None else second + b
        return first, second

    def z_part(one, g, opening=False):
        own = terms_of(one, me_sp, conc, depths)
        if opening and g == 0:
            for x in range(rows_x):
                own_mix[0, x], own_mix[1, x] = mixed(own, x)
            depth_pair.wait_recv()
        others = terms_of(one, 1 - me_sp, other, other_depths)
        parts = 2 if opening else 1
        modes = [[], []]
        for i in range(parts):
            if opening:
                pair[2 * g + i].wait_recv()
            bulk_mix, conc_mix = [], []
            for block in range(i * blocks // parts, (i + 1) * blocks // parts):
                x = g * blocks + block
                if opening:
                    first, second = mixed(others, x, own_mix[0, x], own_mix[1, x])
                else:
                    first, second = mixed(own + others, x)
                bulk_mix.append(first)
                conc_mix.append(second)
            lines = from_right(jnp.concatenate(bulk_mix + conc_mix, axis=0), right_f[...])
            lines = lines.reshape(2, blocks // parts, rows_y, n)
            for f in range(2):
                modes[f] += [lines[f, block] for block in range(blocks // parts)]
        for f in range(2):
            swapped = swap_blocks(modes[f], width)
            for block in range(blocks):
                unit = PIECES * one + block % PIECES
                z_out[2 * unit + f, block // PIECES, g] = swapped[block]
            if opening:
                for peer in others_pz:
                    z_copy(f, peer, pl.ds(g, 1)).start()
        if g == groups - 1:
            for c in range(2 if opening else 0, 2 * PIECES):
                for peer in others_pz:
                    z_copy(2 * PIECES * one + c, peer, pl.ds(0, groups)).start()
            for c in range(2 * PIECES):
                chunk = 2 * PIECES * one + c
                z_in[chunk, :, y_rows] = z_out[chunk, me_pz]

    def y_chunk(chunk):
        for g in range(0, groups, 2):
            lines = jnp.concatenate([z_in[chunk, g], z_in[chunk, g + 1]], axis=1)
            modes = from_left(left_f[...], lines)
            for h in range(2):
                part = modes[:, h * n : (h + 1) * n].reshape(blocks, sub, n)
                swapped = swap_blocks([part[b] for b in range(blocks)], width)
                for block in range(blocks):
                    x = (g + h) * blocks + block
                    y_out[chunk, pl.ds(x, sub, stride=rows_x), :] = swapped[block]

    def y_send(one):
        @pl.when(outer)
        def _():
            for q in range(quarters):
                for f in range(2):
                    y_copy(one, f, q).start()

    def square(index):
        freq = jnp.minimum(index, n - index).astype(jnp.float32)
        root = freq * (2.0 * math.pi / n)
        return root * root

    lane = lax.broadcasted_iota(jnp.int32, (1, n), 1)
    ksq_x = square(lax.broadcasted_iota(jnp.int32, (n, 1), 0))

    def x_quarter(one, q):
        y_all(one, q).wait_recv()
        own_i = me_sp * species + one // PIECES
        piece = me_pz * PIECES + lax.rem(one, PIECES)
        ksq_z = square(piece * width + lane % width)
        half_stiff = 0.5 * (mobility[own_i, own_i] * kappa[own_i])

        def line_rows(h):
            return pl.ds(pl.multiple_of((2 * q + h) * rows_x, rows_x), rows_x)

        both, ksq = [], []
        for f in range(2):
            chunk = 2 * one + f
            both.append(from_left(half_f[...], jnp.concatenate([
                jnp.concatenate([
                    field[chunk, line_rows(h), :] for field in (y_out, y_in)
                ], axis=0)
                for h in range(2)
            ], axis=1)))
        for h in range(2):
            ksq_y = square((lane // width) * sub + (2 * q + h))
            ksq.append(ksq_x + (ksq_y + ksq_z))
        ksq = jnp.concatenate(ksq, axis=1)
        drop = 0.5 * ksq * (both[0] + ksq * both[1]) / (1.0 + half_stiff * (ksq * ksq))
        lines = from_left(half_i[...], drop)
        for h in range(2):
            for i, (field, part) in enumerate([(near, 0), (near, 1), (x_out, 0), (x_out, 1)]):
                field[one, part, line_rows(h), :] = lines[
                    i * rows_x : (i + 1) * rows_x, h * n : (h + 1) * n
                ]
        x_copy(one, 1, q).start()
        x_copy(one, 0, q).start()

        @pl.when(one * quarters + q >= units * quarters - DIRECT)
        def _():
            rows = rows_of(q)
            remote(
                near.at[last, 1, rows], b_in.at[last, rows], b_sent, br.at[last % SLOTS], buddy
            ).start()

    def combine_quarter(step):
        one, q = step // quarters, lax.rem(step, quarters)
        rows = rows_of(q)
        x_copy(one, 1, q).wait_recv()
        b_out[one, rows, :] = near[one, 1, rows, :] + x_in[one, 1, rows, :]
        remote(
            b_out.at[one, rows], b_in.at[one, rows], b_sent, br.at[slot_of(one)], buddy
        ).start()

    def combine_inner(one):
        x_all(one).wait_recv()
        b_in[one] = near[one, 0] + x_in[one, 0]

    def y_back(one, closing=False):
        for g in range(0, groups, 2):
            pairs = []
            for h in range(2):
                parts = []
                for block in range(blocks):
                    x = (g + h) * blocks + block
                    parts.append(b_in[one, pl.ds(x, sub, stride=rows_x), :])
                swapped = swap_blocks(parts, width)
                pairs.append(jnp.stack(swapped, axis=0).reshape(n, n))
            lines = from_left(left_i[...], jnp.concatenate(pairs, axis=1))
            for h in range(2):
                part = lines[:, h * n : (h + 1) * n].reshape(count_pz, rows_y, n)
                w_out[one, :, g + h] = part
        if closing:
            for g in range(groups):
                for peer in others_pz:
                    w_copy(one, peer, pl.ds(g, 1), species + g).start()
        else:
            for peer in others_pz:
                w_copy(one, peer, pl.ds(0, groups), one // PIECES).start()
        w_in[one, me_pz] = w_out[one, me_pz]

    def back(one):
        @pl.when(inner)
        def _():
            combine_inner(one)

        @pl.when(outer)
        def _():
            b_all(one).wait_recv()

        y_back(one)

    def z_back(one, closing=False):
        w_all(one, PIECES - 1 if closing else PIECES).wait_recv()
        if closing:
            for g in range(groups):
                w_last(g).wait_recv()
        for g in range(groups):
            rows = swap_blocks([
                w_in[PIECES * one + block % PIECES, block // PIECES, g]
                for block in range(blocks)
            ], width)
            lines = from_right(jnp.concatenate(rows, axis=0), right_i[...])
            lines = lines.reshape(blocks, rows_y, n)
            for block in range(blocks):
                x = g * blocks + block
                out[one, x] = conc[one, x] - lines[block]

    table_loads[0].wait()
    for g in range(groups):
        z_part(0, g, True)
    for copy in table_loads[1:]:
        copy.wait()
    for g in range(groups):
        z_part(1, g)
    for f in range(2):
        z_all(f, 1, f).wait_recv()
        y_chunk(f)

        @pl.when(outer)
        def _(f=f):
            for q in range(EARLY):
                y_copy(0, f, q).start()

    @pl.when(outer)
    def _():
        for q in range(EARLY, quarters):
            for f in range(2):
                y_copy(0, f, q).start()

    z_all(2, 2, 2).wait_recv()
    for f in range(2):
        y_chunk(2 + f)
    y_send(1)
    extra = {}
    for one in range(2, species):
        for g in range(groups):
            extra[2 + (one - 2) * groups + g] = functools.partial(z_part, one, g)
    for one in range(species - 1):
        extra[units + 1 - 2 * (species - 1 - one)] = functools.partial(z_back, one)

    def middle(step, _):
        one, q = step // quarters, lax.rem(step, quarters)
        ahead, behind = one + 2, one - 2

        @pl.when(jnp.logical_and(inner, step >= LAG))
        def _():
            combine_quarter(step - LAG)

        @pl.when(inner)
        def _():
            x_quarter(one, q)

        for unit, work in extra.items():
            @pl.when(jnp.logical_and(one == unit, q == 0))
            def _(work=work):
                work()

        @pl.when(jnp.logical_and(ahead < 2 * PIECES, q == 1))
        def _():
            z_all(2 * ahead, 2, ahead + 1).wait_recv()

        for each in range(2, species):
            @pl.when(jnp.logical_and(ahead == PIECES * each, q == 1))
            def _(each=each):
                z_all(2 * PIECES * each, 2 * PIECES, 2 * PIECES - 1 + each).wait_recv()

        @pl.when(jnp.logical_and(ahead < units, jnp.logical_and(q > 0, q < 3)))
        def _():
            y_chunk(2 * ahead + q - 1)

        @pl.when(jnp.logical_and(ahead < units, q == 2))
        def _():
            y_send(ahead)

        @pl.when(jnp.logical_and(behind >= 0, q == 3))
        def _():
            back(behind)

        return 0

    steps = units * quarters
    lax.fori_loop(0, steps, middle, 0)

    def returns(step, _):
        combine_quarter(step)
        return 0

    @pl.when(inner)
    def _():
        lax.fori_loop(steps - LAG, steps - quarters, returns, 0)

    back(last - 1)

    @pl.when(inner)
    def _():
        lax.fori_loop(steps - quarters, steps - DIRECT, returns, 0)
        combine_inner(last)

    @pl.when(outer)
    def _():
        b_all(last).wait_recv()
        for q in range(quarters - DIRECT, quarters):
            x_copy(last, 1, q).wait_recv()
            rows = rows_of(q)
            b_in[last, rows, :] = b_in[last, rows, :] + x_in[last, 1, rows, :]

    y_back(last, True)
    z_back(species - 1, True)

    depth_pair.wait_send()
    waiter(conc, pair_sent.at[0]).wait_send()
    waiter(z_out.at[:, pl.ds(0, count_pz - 1)], z_sent).wait_send()

    @pl.when(outer)
    def _():
        waiter(y_out, y_sent).wait_send()

    @pl.when(inner)
    def _():
        waiter(x_out, x_sent).wait_send()
        waiter(b_out, b_sent).wait_send()

    waiter(w_out.at[:, pl.ds(0, count_pz - 1)], w_sent).wait_send()


def per_device_kernel(concentration, mobility, kappa, well_depth):
    species, rows_x, rows_y, n = concentration.shape
    count_py, count_pz = lax.axis_size("py"), lax.axis_size("pz")
    table = basis(n)
    forward = split_table(table)
    inverse = split_table(table.T)
    square_tables = np.stack([forward, forward.T, inverse.T, inverse])
    blocks = np.arange(n).reshape(count_py, rows_x)
    orders = [blocks[[1, 0, 2, 3]].reshape(n), blocks[[2, 3, 1, 0]].reshape(n)]
    half_forward = np.stack([split_table(table[order[: n // 2]]).T for order in orders])
    half_inverse = np.stack([split_table(table[order].T).T for order in orders])
    blocks = count_pz * PIECES
    units = species * PIECES
    groups = rows_x // blocks
    strip = rows_x * SUBLANES
    f32, bf16 = jnp.float32, jnp.bfloat16
    hbm = pl.BlockSpec(memory_space=pltpu.HBM)
    dma = pltpu.SemaphoreType.DMA

    def far(array):
        return pltpu.with_memory_space_constraint(array, pltpu.HBM)

    return pl.pallas_call(
        kernel,
        out_shape=jax.ShapeDtypeStruct(concentration.shape, f32),
        in_specs=[hbm] * 7,
        out_specs=pl.BlockSpec(memory_space=pltpu.VMEM),
        scratch_shapes=[
            pltpu.SMEM(mobility.shape, f32),
            pltpu.SMEM(kappa.shape, f32),
            pltpu.SMEM(well_depth.shape, f32),
            pltpu.VMEM((species, rows_x, rows_y, n), f32),
            pltpu.VMEM(square_tables.shape, bf16),
            pltpu.VMEM(half_forward.shape[1:], bf16),
            pltpu.VMEM(half_inverse.shape[1:], bf16),
            pltpu.VMEM((2, rows_x, rows_y, n), f32),
            pltpu.VMEM((species, rows_x, rows_y, n), f32),
            pltpu.VMEM((species, n), f32),
            pltpu.VMEM((species, n), f32),
            pltpu.VMEM((2 * units, count_pz, groups, rows_y, n), f32),
            pltpu.VMEM((2 * units, groups, n, n), f32),
            pltpu.VMEM((2 * units, strip, n), f32),
            pltpu.VMEM((2 * units, strip, n), f32),
            pltpu.VMEM((units, 2, strip, n), f32),
            pltpu.VMEM((units, 2, strip, n), f32),
            pltpu.VMEM((units, 2, strip, n), f32),
            pltpu.VMEM((units, strip, n), f32),
            pltpu.VMEM((units, strip, n), f32),
            pltpu.VMEM((units, count_pz, groups, rows_y, n), f32),
            pltpu.VMEM((units, count_pz, groups, rows_y, n), f32),
            dma((groups + 6,)), dma((2,)), dma((2 * groups + 1,)), dma((5,)),
            dma((2 * PIECES + species - 1,)), dma((SLOTS, SUBLANES // 2)), dma((SLOTS + 1 + STEPS,)), dma((SLOTS,)),
            dma((species + groups,)),
        ],
        compiler_params=pltpu.CompilerParams(
            collective_id=0, has_side_effects=True, vmem_limit_bytes=46 * 1024 * 1024
        ),
        name="step",
    )(*(
        far(jnp.asarray(each)) for each in (
            concentration, mobility, kappa, well_depth, square_tables, half_forward, half_inverse
        )
    ))


def per_device(concentration, mobility, kappa, well_depth):
    species, rows_x, rows_y, n = concentration.shape
    count_sp, count_py, count_pz = (lax.axis_size(name) for name in ("sp", "py", "pz"))
    cube = rows_x * count_py == n and rows_y * count_pz == n and n == 128
    blocks = count_pz * PIECES
    whole = n == SUBLANES * blocks and rows_x % (2 * blocks) == 0 and rows_y % SUBLANES == 0
    if cube and whole and count_sp == 2 and count_py == 4 and count_pz == 4 and species == 4:
        return per_device_kernel(concentration, mobility, kappa, well_depth)
    return per_device_general(concentration, mobility, kappa, well_depth)


def solution(mesh):
    in_specs = (P("sp", "py", "pz", None), P(), P(), P("sp"))
    out_specs = P("sp", "py", "pz", None)
    return jax.shard_map(
        per_device, mesh=mesh, in_specs=in_specs, out_specs=out_specs, check_vma=False
    )
```
